128 devices in a mesh: pod: 1, dp: 128 (over z, y, x, core).
Axes of the slice: x: 4, y: 4, z: 4, core: 2. Of those that a mesh axis runs over, the one named last changes fastest.
Arguments:
- tok_ids: int32 [131072], P(('pod', 'dp'))
- seg_ids: int32 [131072], P(('pod', 'dp'))
- positions: int32 [131072], P(('pod', 'dp'))
- emb_table: bfloat16 [102400, 512], P('dp')
- gain_emb: bfloat16 [512], P('dp')
- w_qkv: bfloat16 [4, 512, 1536], P(None, 'dp')
- w_out: bfloat16 [4, 512, 512], P(None, 'dp')
- w_in: bfloat16 [4, 512, 4096], P(None, 'dp')
- w_down: bfloat16 [4, 2048, 512], P(None, 'dp')
- gain_attn: bfloat16 [3, 512], P(None, 'dp')
- gain_mlp: bfloat16 [4, 512], P(None, 'dp')
- gain_final: bfloat16 [512], P('dp')
Outputs:
- output: float32 [4096, 512], P(('pod', 'dp'))
All inputs are finite; a program needn't handle non-finite values.
Results may differ from the reference program's by a relative error of at most 0.0195434.
Values are sent between devices in bfloat16 or wider.
A program may use at most 1 GiB of HBM per device.

```python
import jax
import jax.numpy as jnp
from jax import lax

VOCAB_SIZE = 102400
D_MODEL = 512
FF_DIM = 2048
CAPACITY = 1024
GROUP_DEVS = 128
MAX_DOCS = 16
DOC_SLOTS = 32
NUM_LAYERS = 4
HEAD_DIM = 64
WINDOW_HALF = 64
QUERY_BLOCK = 128
NUM_HEADS = D_MODEL // HEAD_DIM
LN_EPS = 1e-5
THETA_GLOBAL = 160000.0
THETA_LOCAL = 10000.0
NEG_BIG = -1e30


def draw_layout(layout_key):
    key_real, key_docs, key_wts, key_first, key_tok = jax.random.split(layout_key, 5)
    dev_index = jnp.arange(GROUP_DEVS)
    n_real = jax.random.randint(key_real, (GROUP_DEVS,), CAPACITY // 2, CAPACITY + 1)
    n_real = jnp.where(dev_index == 1, CAPACITY, n_real)
    n_docs = jax.random.randint(key_docs, (GROUP_DEVS,), max(1, MAX_DOCS // 4), MAX_DOCS + 1)
    n_docs = jnp.where(dev_index == 0, MAX_DOCS, n_docs)
    doc_wts = jax.random.randint(key_wts, (GROUP_DEVS, MAX_DOCS), 1, 17)
    doc_wts = jnp.where(jnp.arange(MAX_DOCS)[None, :] < n_docs[:, None], doc_wts, 0)
    cum_wts = jnp.cumsum(doc_wts, axis=1)
    doc_ends = n_real[:, None] * cum_wts // cum_wts[:, -1:]
    slot_index = jnp.arange(CAPACITY)
    passed = doc_ends[:, None, :] <= slot_index[None, :, None]
    is_real = slot_index[None, :] < n_real[:, None]
    seg_ids = jnp.where(is_real, jnp.sum(passed.astype(jnp.int32), axis=2), -1)
    doc_start = jnp.max(jnp.where(passed, doc_ends[:, None, :], 0), axis=2)
    positions = jnp.where(is_real, slot_index[None, :] - doc_start, 0)
    shard_rows = VOCAB_SIZE // GROUP_DEVS
    tok_ids = jax.random.randint(key_tok, (GROUP_DEVS, CAPACITY), 0, VOCAB_SIZE)
    first_ids = dev_index * shard_rows + jax.random.randint(key_first, (GROUP_DEVS,), 0, shard_rows)
    tok_ids = tok_ids.at[:, 0].set(first_ids)
    return (tok_ids.reshape(-1).astype(jnp.int32), seg_ids.reshape(-1).astype(jnp.int32), positions.reshape(-1).astype(jnp.int32))


def setup_inputs(seed: int = 0, part: int = 0) -> dict:
    shared_key, part_key = jax.random.split(jax.random.key(seed))
    tok_ids, seg_ids, positions = draw_layout(jax.random.fold_in(part_key, part))
    weight_keys = jax.random.split(shared_key, 9)

    def normal_bf16(key_w, shape_w, scale):
        return (jax.random.normal(key_w, shape_w, jnp.float32) * scale).astype(jnp.bfloat16)

    def gain_bf16(key_g, shape_g):
        return (1.0 + 0.3 * jax.random.normal(key_g, shape_g, jnp.float32)).astype(jnp.bfloat16)

    return {
        "tok_ids": tok_ids,
        "seg_ids": seg_ids,
        "positions": positions,
        "emb_table": normal_bf16(weight_keys[0], (VOCAB_SIZE, D_MODEL), 1.0),
        "gain_emb": gain_bf16(weight_keys[1], (D_MODEL,)),
        "w_qkv": normal_bf16(weight_keys[2], (NUM_LAYERS, D_MODEL, 3 * D_MODEL), D_MODEL ** -0.5),
        "w_out": normal_bf16(weight_keys[3], (NUM_LAYERS, D_MODEL, D_MODEL), D_MODEL ** -0.5),
        "w_in": normal_bf16(weight_keys[4], (NUM_LAYERS, D_MODEL, 2 * FF_DIM), D_MODEL ** -0.5),
        "w_down": normal_bf16(weight_keys[5], (NUM_LAYERS, FF_DIM, D_MODEL), FF_DIM ** -0.5),
        "gain_attn": gain_bf16(weight_keys[6], (NUM_LAYERS - 1, D_MODEL)),
        "gain_mlp": gain_bf16(weight_keys[7], (NUM_LAYERS, D_MODEL)),
        "gain_final": gain_bf16(weight_keys[8], (D_MODEL,)),
    }


def layer_norm(values, gain):
    as_float = values.astype(jnp.float32)
    centered = as_float - jnp.mean(as_float, axis=-1, keepdims=True)
    variance = jnp.mean(centered * centered, axis=-1, keepdims=True)
    return centered * lax.rsqrt(variance + LN_EPS) * gain.astype(jnp.float32)


def rope_tables(positions, theta):
    inv_freq = theta ** (-jnp.arange(0, HEAD_DIM, 2).astype(jnp.float32) / HEAD_DIM)
    angles = positions.astype(jnp.float32)[:, None] * inv_freq[None, :]
    angles = jnp.concatenate([angles, angles], axis=-1)
    return jnp.cos(angles), jnp.sin(angles)


def apply_rope(heads_in, tables):
    cos_tab, sin_tab = tables
    half_dim = HEAD_DIM // 2
    as_float = heads_in.astype(jnp.float32)
    rotated = jnp.concatenate([-as_float[..., half_dim:], as_float[..., :half_dim]], axis=-1)
    return (as_float * cos_tab[:, None, :] + rotated * sin_tab[:, None, :]).astype(jnp.bfloat16)


def attend(queries, keys_rot, values_in, seg_ids, positions, is_local):
    n_blocks = CAPACITY // QUERY_BLOCK
    keys_f = keys_rot.astype(jnp.float32)
    values_f = values_in.astype(jnp.float32)
    key_ok = seg_ids != -1

    def one_block(block_args):
        q_blk, seg_blk, pos_blk = block_args
        scores = jnp.einsum("qhd,khd->hqk", q_blk.astype(jnp.float32), keys_f) * (HEAD_DIM ** -0.5)
        allowed = (seg_blk[:, None] == seg_ids[None, :]) & key_ok[None, :]
        if is_local:
            allowed = allowed & (jnp.abs(pos_blk[:, None] - positions[None, :]) <= WINDOW_HALF)
        scores = jnp.where(allowed[None], scores, NEG_BIG)
        probs = jax.nn.softmax(scores, axis=-1).astype(jnp.bfloat16)
        ctx_blk = jnp.einsum("hqk,khd->qhd", probs.astype(jnp.float32), values_f)
        return ctx_blk.astype(jnp.bfloat16)

    blocks = lax.map(one_block, (queries.reshape(n_blocks, QUERY_BLOCK, NUM_HEADS, HEAD_DIM), seg_ids.reshape(n_blocks, QUERY_BLOCK), positions.reshape(n_blocks, QUERY_BLOCK)))
    return blocks.reshape(CAPACITY, D_MODEL)


def reference(tok_ids, seg_ids, positions, emb_table, gain_emb, w_qkv, w_out, w_in, w_down, gain_attn, gain_mlp, gain_final):
    def encode_device(dev_args):
        dev_tok, dev_seg, dev_pos = dev_args
        hidden = layer_norm(jnp.take(emb_table, dev_tok, axis=0), gain_emb).astype(jnp.bfloat16)
        rope_global = rope_tables(dev_pos, THETA_GLOBAL)
        rope_local = rope_tables(dev_pos, THETA_LOCAL)
        for layer_idx in range(NUM_LAYERS):
            is_local = layer_idx % 3 != 0
            if layer_idx == 0:
                attn_in = hidden
            else:
                attn_in = layer_norm(hidden, gain_attn[layer_idx - 1]).astype(jnp.bfloat16)
            qkv_proj = jnp.dot(attn_in, w_qkv[layer_idx], preferred_element_type=jnp.float32).astype(jnp.bfloat16)
            qkv_proj = qkv_proj.reshape(CAPACITY, 3, NUM_HEADS, HEAD_DIM)
            tables = rope_local if is_local else rope_global
            context = attend(apply_rope(qkv_proj[:, 0], tables), apply_rope(qkv_proj[:, 1], tables), qkv_proj[:, 2], dev_seg, dev_pos, is_local)
            attn_out = jnp.dot(context, w_out[layer_idx], preferred_element_type=jnp.float32)
            hidden = (hidden.astype(jnp.float32) + attn_out).astype(jnp.bfloat16)
            mlp_in = layer_norm(hidden, gain_mlp[layer_idx]).astype(jnp.bfloat16)
            pre_act = jnp.dot(mlp_in, w_in[layer_idx], preferred_element_type=jnp.float32)
            gated_act = (jax.nn.gelu(pre_act[:, :FF_DIM], approximate=False) * pre_act[:, FF_DIM:]).astype(jnp.bfloat16)
            mlp_out = jnp.dot(gated_act, w_down[layer_idx], preferred_element_type=jnp.float32)
            hidden = (hidden.astype(jnp.float32) + mlp_out).astype(jnp.bfloat16)
        final_f = layer_norm(hidden, gain_final)
        member = (dev_seg[None, :] == jnp.arange(DOC_SLOTS)[:, None]).astype(jnp.float32)
        doc_sums = jnp.dot(member, final_f, preferred_element_type=jnp.float32)
        doc_counts = jnp.sum(member, axis=1)
        return doc_sums / jnp.maximum(doc_counts, 1.0)[:, None]

    pooled = lax.map(encode_device, (tok_ids.reshape(GROUP_DEVS, CAPACITY), seg_ids.reshape(GROUP_DEVS, CAPACITY), positions.reshape(GROUP_DEVS, CAPACITY)))
    return pooled.reshape(GROUP_DEVS * DOC_SLOTS, D_MODEL)
```

```python
import functools

import jax
import jax.numpy as jnp
from jax import lax
from jax.experimental import pallas as pl
from jax.experimental.pallas import tpu as pltpu
from jax.sharding import PartitionSpec as P

D_MODEL = 512
FF_DIM = 2048
N_LAYERS = 4
N_SLOTS = 1024
HEAD_DIM = 64
N_PAIRS = 4
WINDOW_HALF = 64
DOC_SLOTS = 32
LN_EPS = 1e-5
THETA_GLOBAL = 160000.0
THETA_LOCAL = 10000.0
NEG_BIG = -1e30
CAP = 24
QB = 128
ROWS = 256
LAYER_COLS = 3 * D_MODEL + D_MODEL + 2 * FF_DIM + FF_DIM
SPANS = (256, 384, 512, 768, 1024)
F32 = jnp.float32
BF16 = jnp.bfloat16


def ln_rows(as_float, gain_row):
    centered = as_float - jnp.mean(as_float, axis=-1, keepdims=True)
    variance = jnp.mean(centered * centered, axis=-1, keepdims=True)
    return centered * lax.rsqrt(variance + LN_EPS) * gain_row


def layer_kernel(layer, lo_ref, kind_ref, x_ref, segc_ref, segr_ref, segs_ref, cos_ref, sin_ref, gain_ref, w_ref, *rest):
    is_first, is_last, is_local = layer == 0, layer == N_LAYERS - 1, layer % 3 != 0
    if is_last:
        out_ref, wq, wo, wi, wd, q_s, k_s, v_s, c_s, z_s, x_s, sems = rest
    else:
        out_ref, wq, wo, wi, wd, q_s, k_s, v_s, c_s, z_s, sems = rest
        x_s = out_ref
    base = layer * LAYER_COLS
    copies = [
        pltpu.make_async_copy(w_ref.at[:, pl.ds(base, 1536)], wq, sems.at[0]),
        pltpu.make_async_copy(w_ref.at[:, pl.ds(base + 1536, 512)], wo, sems.at[1]),
        pltpu.make_async_copy(w_ref.at[:, pl.ds(base + 2048, 4096)], wi, sems.at[2]),
    ] + [pltpu.make_async_copy(w_ref.at[:, pl.ds(base + 6144 + 512 * j, 512)], wd.at[j], sems.at[3 + j]) for j in range(4)]
    for copy in copies:
        copy.start()
    pad = WINDOW_HALF
    if is_local:
        zeros = jnp.zeros((pad, 128), BF16)
        for pair in range(N_PAIRS):
            for ref in (k_s, v_s):
                ref[pair, pl.ds(0, pad), :] = zeros
                ref[pair, pl.ds(pad + N_SLOTS, pad), :] = zeros
    lane = lax.broadcasted_iota(jnp.int32, (1, 128), 1)
    low_half = (lane % HEAD_DIM) < HEAD_DIM // 2
    first_head = lane < HEAD_DIM
    copies[0].wait()

    @pl.loop(0, N_SLOTS // ROWS)
    def qkv_rows(block):
        rows = pl.ds(pl.multiple_of(block * ROWS, ROWS), ROWS)
        prows = pl.ds(pl.multiple_of(block * ROWS + pad, pad), ROWS)
        x = x_ref[rows, :]
        if is_first:
            u = ln_rows(x.astype(F32), gain_ref[0:1, :]).astype(BF16)
            x_s[rows, :] = u
        else:
            u = ln_rows(x.astype(F32), gain_ref[1 + layer:2 + layer, :]).astype(BF16)
        cos_t, sin_t = cos_ref[rows, :], sin_ref[rows, :]

        def rope(cols):
            h = jnp.dot(u, wq[:, cols:cols + 128], preferred_element_type=F32).astype(BF16).astype(F32)
            turned = jnp.where(low_half, pltpu.roll(h, 96, 1), pltpu.roll(h, 32, 1))
            return h * cos_t + turned * sin_t

        for pair in range(N_PAIRS):
            q = rope(pair * 128)
            q_s[0, pair, rows, :] = jnp.where(first_head, q, 0.0).astype(BF16)
            q_s[1, pair, rows, :] = jnp.where(first_head, 0.0, q).astype(BF16)
            k_s[pair, prows, :] = rope(512 + pair * 128).astype(BF16)
        v = jnp.dot(u, wq[:, 1024:1536], preferred_element_type=F32).astype(BF16)
        for pair in range(N_PAIRS):
            v_s[pair, prows, :] = v[:, pair * 128:(pair + 1) * 128]

    def attend(qrows, krows, allowed):
        for pair in range(N_PAIRS):
            kk = k_s[pair, krows, :]
            vv = v_s[pair, krows, :]
            halves = []
            for half in range(2):
                s = lax.dot_general(q_s[half, pair, qrows, :], kk, (((1,), (1,)), ((), ())), preferred_element_type=F32)
                s = jnp.where(allowed, s, NEG_BIG)
                e = jnp.exp((s - jnp.max(s, axis=1, keepdims=True)) * (HEAD_DIM ** -0.5))
                p = (e * (1.0 / jnp.sum(e, axis=1, keepdims=True))).astype(BF16)
                halves.append(jnp.dot(p, vv, preferred_element_type=F32))
            c_s[qrows, pair * 128:(pair + 1) * 128] = jnp.where(first_head, halves[0], halves[1]).astype(BF16)

    if is_local:
        qi = lax.broadcasted_iota(jnp.int32, (QB, 2 * QB), 0)
        kj = lax.broadcasted_iota(jnp.int32, (QB, 2 * QB), 1)
        band = (kj >= qi) & (kj - qi <= 2 * WINDOW_HALF)

        @pl.loop(0, N_SLOTS // QB)
        def local_block(block):
            start = pl.multiple_of(block * QB, QB)
            qrows = pl.ds(start, QB)
            allowed = (segc_ref[qrows, :] == segs_ref[:, pl.ds(start, 2 * QB)]) & band
            attend(qrows, pl.ds(start, 2 * QB), allowed)
    else:
        @pl.loop(0, N_SLOTS // QB)
        def global_block(block):
            qrows = pl.ds(pl.multiple_of(block * QB, QB), QB)
            kind = kind_ref[block]
            for index, span in enumerate(SPANS):
                @pl.when(kind == index)
                def run():
                    k0 = jnp.minimum(lo_ref[block] * QB, N_SLOTS - span)
                    kcols = pl.ds(pl.multiple_of(k0, QB), span)
                    allowed = segc_ref[qrows, :] == segr_ref[:, kcols]
                    attend(qrows, pl.ds(pl.multiple_of(k0 + pad, pad), span), allowed)

    for copy in copies[1:]:
        copy.wait()

    @pl.loop(0, N_SLOTS // ROWS)
    def mlp_rows(block):
        rows = pl.ds(pl.multiple_of(block * ROWS, ROWS), ROWS)
        attn = jnp.dot(c_s[rows, :], wo[...], preferred_element_type=F32)
        x = x_s[rows, :] if is_first else x_ref[rows, :]
        hidden = (x.astype(F32) + attn).astype(BF16)
        m = ln_rows(hidden.astype(F32), gain_ref[5 + layer:6 + layer, :]).astype(BF16)
        for j in range(8):
            a = jnp.dot(m, wi[:, j * 256:(j + 1) * 256], preferred_element_type=F32)
            b = jnp.dot(m, wi[:, FF_DIM + j * 256:FF_DIM + (j + 1) * 256], preferred_element_type=F32)
            gelu = 0.5 * a * (1.0 + lax.erf(a * (0.5 ** 0.5)))
            z_s[:, j * 256:(j + 1) * 256] = (gelu * b).astype(BF16)
        down = jnp.dot(z_s[...], wd[...].reshape(FF_DIM, D_MODEL), preferred_element_type=F32)
        x_s[rows, :] = (hidden.astype(F32) + down).astype(BF16)

    if is_last:
        docs = lax.broadcasted_iota(jnp.int32, (DOC_SLOTS, N_SLOTS), 0)
        member = (docs == segr_ref[...]).astype(F32)
        f = ln_rows(x_s[...].astype(F32), gain_ref[9:10, :])
        sums = jnp.dot(member, f, precision=lax.Precision.HIGHEST, preferred_element_type=F32)
        out_ref[...] = sums / jnp.maximum(jnp.sum(member, axis=1, keepdims=True), 1.0)


def run_layer(layer, lo, kind, x, segc, segr, segs, cos_t, sin_t, gains, weights):
    is_last = layer == N_LAYERS - 1
    vmem = pl.BlockSpec(memory_space=pltpu.VMEM)
    smem = pl.BlockSpec(memory_space=pltpu.SMEM)
    scratch = [
        pltpu.VMEM((512, 1536), BF16), pltpu.VMEM((512, 512), BF16), pltpu.VMEM((512, 4096), BF16), pltpu.VMEM((4, 512, 512), BF16),
        pltpu.VMEM((2, N_PAIRS, N_SLOTS, 128), BF16), pltpu.VMEM((N_PAIRS, N_SLOTS + 128, 128), BF16),
        pltpu.VMEM((N_PAIRS, N_SLOTS + 128, 128), BF16), pltpu.VMEM((N_SLOTS, 512), BF16), pltpu.VMEM((ROWS, FF_DIM), BF16),
    ]
    if is_last:
        out_shape = jax.ShapeDtypeStruct((DOC_SLOTS, D_MODEL), F32)
        scratch.append(pltpu.VMEM((N_SLOTS, D_MODEL), BF16))
    else:
        out_shape = jax.ShapeDtypeStruct((N_SLOTS, D_MODEL), BF16)
    scratch.append(pltpu.SemaphoreType.DMA((7,)))
    return pl.pallas_call(
        functools.partial(layer_kernel, layer),
        out_shape=out_shape,
        in_specs=[smem, smem] + [vmem] * 7 + [pl.BlockSpec(memory_space=pl.ANY)],
        out_specs=vmem,
        scratch_shapes=scratch,
        compiler_params=pltpu.CompilerParams(vmem_limit_bytes=48 * 2 ** 20),
        cost_estimate=pl.CostEstimate(flops=10 ** 10, bytes_accessed=10 ** 7, transcendentals=10 ** 7),
        name=f"layer_{layer}",
    )(lo, kind, x, segc, segr, segs, cos_t, sin_t, gains, weights)


def pack_shard(gain_emb, w_qkv, w_out, w_in, w_down, gain_attn, gain_mlp, gain_final):
    src = jnp.arange(512)
    dst = ((src // 4) % 4) * 128 + (src // 16) * 4 + src % 4
    perm = (dst[:, None] == jnp.arange(512)[None, :]).astype(BF16)
    cols = jnp.dot(w_in.reshape(128, 512), perm, preferred_element_type=F32).astype(BF16)
    cols = cols.reshape(N_LAYERS * 4 * 2, 4, 4, 128).transpose(0, 2, 1, 3).reshape(N_LAYERS, 4, 2 * FF_DIM)
    down = w_down.reshape(N_LAYERS, 4, 4, 512).transpose(0, 2, 1, 3).reshape(N_LAYERS, 4, FF_DIM)
    parts = []
    for layer in range(N_LAYERS):
        parts += [w_qkv[layer], w_out[layer], cols[layer], down[layer]]
    gains = jnp.concatenate([gain_emb[None], gain_emb[None], gain_attn, gain_mlp, gain_final[None]], axis=0)
    parts.append(jnp.pad(gains.T, ((0, 0), (0, 128 - gains.shape[0]))))
    return jnp.concatenate(parts, axis=1)


def embed_rows(tok_ids, seg_ids, table):
    n_dev = lax.axis_size("dp")
    shard_rows = table.shape[0]
    owner = jnp.where(seg_ids >= 0, tok_ids // shard_rows, -1)
    local = tok_ids % shard_rows
    hot = (owner[:, None] == jnp.arange(n_dev)[None, :]).astype(BF16)
    earlier = (jnp.arange(N_SLOTS)[:, None] > jnp.arange(N_SLOTS)[None, :]).astype(BF16)
    before = jnp.dot(earlier, hot, preferred_element_type=F32)
    rank = jnp.sum(before * hot.astype(F32), axis=1).astype(jnp.int32)
    most = jnp.max(jnp.sum(hot.astype(F32), axis=0)).astype(jnp.int32)
    place = rank[:, None] == jnp.arange(CAP)[None, :]
    high = jnp.where(place, (local // 32)[:, None], 0).astype(BF16)
    low = jnp.where(place, (local % 32)[:, None], 0).astype(BF16)
    both = lax.dot_general(hot, jnp.concatenate([high, low], axis=1), (((0,), (0,)), ((), ())), preferred_element_type=F32)
    wanted = (both[:, :CAP] * 32.0 + both[:, CAP:]).astype(jnp.int32)
    message = jnp.concatenate([wanted, jnp.full((n_dev, 128 - CAP), most, jnp.int32)], axis=1)
    asked = lax.all_to_all(message, "dp", split_axis=0, concat_axis=0, tiled=True)
    worst = jnp.max(asked[:, CAP:])
    ask_hot = (asked[:, :CAP].reshape(n_dev * CAP, 1) == jnp.arange(shard_rows)[None, :]).astype(BF16)
    rows = jnp.dot(ask_hot, table, preferred_element_type=F32).astype(BF16).reshape(n_dev, CAP, D_MODEL)
    got = lax.all_to_all(rows, "dp", split_axis=0, concat_axis=0, tiled=True).reshape(n_dev * CAP, D_MODEL)

    def exchanged():
        slot = jnp.where(owner >= 0, owner * CAP + rank, -1)
        pick = (slot[:, None] == jnp.arange(n_dev * CAP)[None, :]).astype(BF16)
        return jnp.dot(pick, got, preferred_element_type=F32).astype(BF16)

    def gathered():
        return jnp.take(lax.all_gather(table, "dp", axis=0, tiled=True), tok_ids, axis=0)

    return lax.cond(worst > CAP, gathered, exchanged)


def rope_tables(positions, theta):
    inv_freq = theta ** (-jnp.arange(0, HEAD_DIM, 2).astype(F32) / HEAD_DIM)
    angles = positions.astype(F32)[:, None] * jnp.tile(inv_freq, 4)[None, :]
    sign = jnp.where(jnp.arange(128) % HEAD_DIM < HEAD_DIM // 2, -1.0, 1.0)
    return jnp.cos(angles), jnp.sin(angles) * sign[None, :]


def key_ranges(seg_ids, positions):
    n_blocks = N_SLOTS // QB
    first = jnp.arange(n_blocks) * QB
    seg_first = seg_ids[::QB]
    lo = jnp.where(seg_first >= 0, first - positions[::QB], first) // QB
    last_seg = jnp.max(seg_ids.reshape(n_blocks, QB), axis=1)
    hi = jnp.sum(((seg_ids >= 0)[None, :] & (seg_ids[None, :] <= last_seg[:, None])).astype(jnp.int32), axis=1)
    span = jnp.maximum(hi - lo * QB, 1)
    kind = jnp.sum((span[:, None] > jnp.array(SPANS)[None, :]).astype(jnp.int32), axis=1)
    return lo.astype(jnp.int32), kind.astype(jnp.int32)


def solution(mesh):
    token_spec = P(("pod", "dp"))
    layer_spec = P(None, "dp", None)
    gain_spec = P(None, "dp")
    in_specs = (token_spec, token_spec, token_spec, P("dp", None), P("dp"), layer_spec, layer_spec, layer_spec, layer_spec, gain_spec, gain_spec, P("dp"))

    def device_program(tok_ids, seg_ids, positions, emb_table, gain_emb, w_qkv, w_out, w_in, w_down, gain_attn, gain_mlp, gain_final):
        shard = pack_shard(gain_emb, w_qkv, w_out, w_in, w_down, gain_attn, gain_mlp, gain_final)
        weights = lax.all_gather(shard, "dp", axis=0, tiled=True)
        hidden = embed_rows(tok_ids, seg_ids, emb_table)
        gains = weights[:, N_LAYERS * LAYER_COLS:N_LAYERS * LAYER_COLS + 16].T.astype(F32)
        seg_key = jnp.where(seg_ids >= 0, seg_ids, -2)
        segc, segr = seg_ids[:, None], seg_key[None, :]
        segs = jnp.pad(segr, ((0, 0), (WINDOW_HALF, WINDOW_HALF)), constant_values=-2)
        lo, kind = key_ranges(seg_ids, positions)
        tables = (rope_tables(positions, THETA_GLOBAL), rope_tables(positions, THETA_LOCAL))
        for layer in range(N_LAYERS):
            cos_t, sin_t = tables[int(layer % 3 != 0)]
            hidden = run_layer(layer, lo, kind, hidden, segc, segr, segs, cos_t, sin_t, gains, weights)
        return hidden

    return jax.shard_map(device_program, mesh=mesh, in_specs=in_specs, out_specs=P(("pod", "dp"), None), check_vma=False)
```

```python
import functools

import jax
import jax.numpy as jnp
from jax import lax
from jax.experimental import pallas as pl
from jax.experimental.pallas import tpu as pltpu
from jax.sharding import PartitionSpec as P

D_MODEL = 512
FF_DIM = 2048
N_LAYERS = 4
N_SLOTS = 1024
HEAD_DIM = 64
N_PAIRS = 4
WINDOW_HALF = 64
DOC_SLOTS = 32
LN_EPS = 1e-5
THETA_GLOBAL = 160000.0
THETA_LOCAL = 10000.0
NEG_BIG = -1e30
N_DEV = 128
ASK = 80
CAP = 16
SPILL = 16
MESH = pl.DeviceIdType.MESH
QB = 128
ROWS = 256
LAYER_COLS = 2048
NEAR_COLS = LAYER_COLS + 256
SPANS = (256, 384, 512, 768, 1024)
F32 = jnp.float32
BF16 = jnp.bfloat16


def ln_rows(as_float, gain_row):
    centered = as_float - jnp.mean(as_float, axis=-1, keepdims=True)
    variance = jnp.mean(centered * centered, axis=-1, keepdims=True)
    return centered * lax.rsqrt(variance + LN_EPS) * gain_row


def layer_kernel(layer, lo_ref, kind_ref, x_ref, segc_ref, segr_ref, segs_ref, cos_ref, sin_ref, gain_ref, w_ref, *rest):
    is_first, is_last, is_local = layer == 0, layer == N_LAYERS - 1, layer % 3 != 0
    if is_last:
        out_ref, w_s, q_s, k_s, v_s, c_s, z_s, x_s, sems = rest
    else:
        out_ref, w_s, q_s, k_s, v_s, c_s, z_s, sems = rest
        x_s = out_ref
    copies = [
        pltpu.make_async_copy(w_ref.at[:, :, layer % 2, :, pl.ds(start, size)], w_s.at[:, :, :, pl.ds(start, size)], sems.at[index])
        for index, (start, size) in enumerate(((0, 384), (384, 128), (512, 1024), (1536, 512)))
    ]
    for copy in copies:
        copy.start()
    pad = WINDOW_HALF
    if is_local:
        zeros = jnp.zeros((pad, 128), BF16)
        for pair in range(N_PAIRS):
            for ref in (k_s, v_s):
                ref[pair, pl.ds(0, pad), :] = zeros
                ref[pair, pl.ds(pad + N_SLOTS, pad), :] = zeros
    lane = lax.broadcasted_iota(jnp.int32, (1, 128), 1)
    low_half = (lane % HEAD_DIM) < HEAD_DIM // 2
    first_head = lane < HEAD_DIM

    def weight(quarter, start, size):
        return w_s[:, quarter, :, start:start + size].reshape(D_MODEL, size)

    copies[0].wait()

    @pl.loop(0, N_SLOTS // ROWS)
    def qkv_rows(block):
        rows = pl.ds(pl.multiple_of(block * ROWS, ROWS), ROWS)
        prows = pl.ds(pl.multiple_of(block * ROWS + pad, pad), ROWS)
        x = x_ref[rows, :]
        if is_first:
            u = ln_rows(x.astype(F32), gain_ref[0:1, :]).astype(BF16)
            x_s[rows, :] = u
        else:
            u = ln_rows(x.astype(F32), gain_ref[layer:layer + 1, :]).astype(BF16)
        cos_t, sin_t = cos_ref[rows, :], sin_ref[rows, :]

        def rope(h):
            h = h.astype(F32)
            turned = jnp.where(low_half, pltpu.roll(h, 96, 1), pltpu.roll(h, 32, 1))
            return h * cos_t + turned * sin_t

        for pair in range(N_PAIRS):
            qkv = jnp.dot(u, weight(pair, 0, 384), preferred_element_type=F32).astype(BF16)
            q = rope(qkv[:, :128])
            q_s[0, pair, rows, :] = jnp.where(first_head, q, 0.0).astype(BF16)
            q_s[1, pair, rows, :] = jnp.where(first_head, 0.0, q).astype(BF16)
            k_s[pair, prows, :] = rope(qkv[:, 128:256]).astype(BF16)
            v_s[pair, prows, :] = qkv[:, 256:]

    def attend(qrows, krows, allowed):
        for pair in range(N_PAIRS):
            kk = k_s[pair, krows, :]
            vv = v_s[pair, krows, :]
            halves = []
            for half in range(2):
                s = lax.dot_general(q_s[half, pair, qrows, :], kk, (((1,), (1,)), ((), ())), preferred_element_type=F32)
                s = jnp.where(allowed, s, NEG_BIG)
                e = jnp.exp((s - jnp.max(s, axis=1, keepdims=True)) * (HEAD_DIM ** -0.5))
                p = (e * (1.0 / jnp.sum(e, axis=1, keepdims=True))).astype(BF16)
                halves.append(jnp.dot(p, vv, preferred_element_type=F32))
            c_s[qrows, pair * 128:(pair + 1) * 128] = jnp.where(first_head, halves[0], halves[1]).astype(BF16)

    if is_local:
        qi = lax.broadcasted_iota(jnp.int32, (QB, 2 * QB), 0)
        kj = lax.broadcasted_iota(jnp.int32, (QB, 2 * QB), 1)
        band = (kj >= qi) & (kj - qi <= 2 * WINDOW_HALF)

        @pl.loop(0, N_SLOTS // QB)
        def local_block(block):
            start = pl.multiple_of(block * QB, QB)
            qrows = pl.ds(start, QB)
            allowed = (segc_ref[qrows, :] == segs_ref[:, pl.ds(start, 2 * QB)]) & band
            attend(qrows, pl.ds(start, 2 * QB), allowed)
    else:
        @pl.loop(0, N_SLOTS // QB)
        def global_block(block):
            qrows = pl.ds(pl.multiple_of(block * QB, QB), QB)
            kind = kind_ref[block]
            for index, span in enumerate(SPANS):
                @pl.when(kind == index)
                def run():
                    k0 = jnp.minimum(lo_ref[block] * QB, N_SLOTS - span)
                    kcols = pl.ds(pl.multiple_of(k0, QB), span)
                    allowed = segc_ref[qrows, :] == segr_ref[:, kcols]
                    attend(qrows, pl.ds(pl.multiple_of(k0 + pad, pad), span), allowed)

    for copy in copies[1:]:
        copy.wait()

    @pl.loop(0, N_SLOTS // ROWS)
    def mlp_rows(block):
        rows = pl.ds(pl.multiple_of(block * ROWS, ROWS), ROWS)
        w_out = jnp.concatenate([weight(quarter, 384, 128) for quarter in range(4)], axis=1)
        attn = jnp.dot(c_s[rows, :], w_out, preferred_element_type=F32)
        x = x_s[rows, :] if is_first else x_ref[rows, :]
        hidden = (x.astype(F32) + attn).astype(BF16)
        m = ln_rows(hidden.astype(F32), gain_ref[4 + layer:5 + layer, :]).astype(BF16)
        for j in range(8):
            quarter, start = j // 2, (j % 2) * 256
            a = jnp.dot(m, weight(quarter, 512 + start, 256), preferred_element_type=F32)
            b = jnp.dot(m, weight(quarter, 1024 + start, 256), preferred_element_type=F32)
            gelu = 0.5 * a * (1.0 + lax.erf(a * (0.5 ** 0.5)))
            z_s[:, j * 256:(j + 1) * 256] = (gelu * b).astype(BF16)
        down = jnp.dot(z_s[...], w_s[:, :, :, 1536:].reshape(FF_DIM, D_MODEL), preferred_element_type=F32)
        x_s[rows, :] = (hidden.astype(F32) + down).astype(BF16)

    if is_last:
        docs = lax.broadcasted_iota(jnp.int32, (DOC_SLOTS, N_SLOTS), 0)
        member = (docs == segr_ref[...]).astype(F32)
        f = ln_rows(x_s[...].astype(F32), gain_ref[8:9, :])
        sums = jnp.dot(member, f, precision=lax.Precision.HIGHEST, preferred_element_type=F32)
        out_ref[...] = sums / jnp.maximum(jnp.sum(member, axis=1, keepdims=True), 1.0)


def run_layer(layer, lo, kind, x, segc, segr, segs, cos_t, sin_t, gains, weights):
    is_last = layer == N_LAYERS - 1
    vmem = pl.BlockSpec(memory_space=pltpu.VMEM)
    smem = pl.BlockSpec(memory_space=pltpu.SMEM)
    scratch = [
        pltpu.VMEM((32, 4, 16, LAYER_COLS), BF16),
        pltpu.VMEM((2, N_PAIRS, N_SLOTS, 128), BF16), pltpu.VMEM((N_PAIRS, N_SLOTS + 128, 128), BF16),
        pltpu.VMEM((N_PAIRS, N_SLOTS + 128, 128), BF16), pltpu.VMEM((N_SLOTS, 512), BF16), pltpu.VMEM((ROWS, FF_DIM), BF16),
    ]
    if is_last:
        out_shape = jax.ShapeDtypeStruct((DOC_SLOTS, D_MODEL), F32)
        scratch.append(pltpu.VMEM((N_SLOTS, D_MODEL), BF16))
    else:
        out_shape = jax.ShapeDtypeStruct((N_SLOTS, D_MODEL), BF16)
    scratch.append(pltpu.SemaphoreType.DMA((4,)))
    return pl.pallas_call(
        functools.partial(layer_kernel, layer),
        out_shape=out_shape,
        in_specs=[smem, smem] + [vmem] * 7 + [pl.BlockSpec(memory_space=pl.ANY)],
        out_specs=vmem,
        scratch_shapes=scratch,
        compiler_params=pltpu.CompilerParams(vmem_limit_bytes=48 * 2 ** 20),
        cost_estimate=pl.CostEstimate(flops=10 ** 10, bytes_accessed=10 ** 7, transcendentals=10 ** 7),
        name=f"layer_{layer}",
    )(lo, kind, x, segc, segr, segs, cos_t, sin_t, gains, weights)


def meet_kernel(say_ref, qkv_ref, out_ref, in_ref, heard_ref, quart_ref, send_sem, recv_sem, own_sem, w_send, w_recv, w_own):
    me = lax.axis_index("dp")
    mine = lax.rem(me, 4)
    barrier = pltpu.get_barrier_semaphore()

    @pl.loop(1, N_DEV)
    def greet(step):
        pl.semaphore_signal(barrier, inc=1, device_id={"dp": lax.rem(me + step, N_DEV)}, device_id_type=MESH)

    own = [pltpu.make_async_copy(say_ref.at[me], heard_ref.at[me], own_sem)]

    def pieces(quarter, slot):
        out = []
        for part in range(3):
            cols = pl.ds(pl.multiple_of(part * 512 + quarter * 128, 128), 128)
            out.append((qkv_ref.at[:, :, cols], quart_ref.at[slot, :, :, pl.ds(part * 128, 128)]))
        out.append((out_ref.at[:, :, pl.ds(pl.multiple_of(quarter * 128, 128), 128)], quart_ref.at[slot, :, :, pl.ds(384, 128)]))
        for part in range(2):
            cols = pl.ds(pl.multiple_of(part * 2048 + quarter * 512, 512), 512)
            out.append((in_ref.at[:, :, cols], quart_ref.at[slot, :, :, pl.ds(512 + part * 512, 512)]))
        return out

    own += [pltpu.make_async_copy(src, dst, w_own.at[index]) for index, (src, dst) in enumerate(pieces(mine, mine))]
    for copy in own:
        copy.start()
    pl.semaphore_wait(barrier, N_DEV - 1)

    quarters = []
    for step in range(1, 4):
        quarter = lax.rem(mine + step, 4)
        for index, (src, dst) in enumerate(pieces(quarter, mine)):
            number = (step - 1) * 6 + index
            quarters.append(pltpu.make_async_remote_copy(
                src_ref=src, dst_ref=dst, send_sem=w_send.at[number], recv_sem=w_recv.at[number],
                device_id={"dp": me - mine + quarter}, device_id_type=MESH))
    for copy in quarters:
        copy.start()

    @pl.loop(1, N_DEV)
    def tell(step):
        peer = lax.rem(me + step, N_DEV)
        pltpu.make_async_remote_copy(
            src_ref=say_ref.at[peer], dst_ref=heard_ref.at[me], send_sem=send_sem, recv_sem=recv_sem,
            device_id={"dp": peer}, device_id_type=MESH).start()

    rest = pltpu.make_async_remote_copy(
        src_ref=say_ref.at[pl.ds(0, N_DEV - 1)], dst_ref=heard_ref.at[pl.ds(0, N_DEV - 1)], send_sem=send_sem, recv_sem=recv_sem,
        device_id={"dp": lax.rem(me + 1, N_DEV)}, device_id_type=MESH)
    rest.wait_send()
    rest.wait_recv()
    for copy in own + quarters:
        copy.wait()


def meet(say, w_qkv, w_out, w_in):
    vmem = pl.BlockSpec(memory_space=pltpu.VMEM)
    dma = pltpu.SemaphoreType.DMA
    return pl.pallas_call(
        meet_kernel,
        out_shape=(jax.ShapeDtypeStruct(say.shape, F32), jax.ShapeDtypeStruct((4, N_LAYERS, 4, 1536), BF16)),
        in_specs=[vmem] * 4,
        out_specs=(vmem, vmem),
        scratch_shapes=[dma, dma, dma, dma((18,)), dma((18,)), dma((6,))],
        compiler_params=pltpu.CompilerParams(collective_id=1, has_side_effects=True),
        cost_estimate=pl.CostEstimate(flops=10 ** 10, bytes_accessed=10 ** 6, transcendentals=0),
        name="meet",
    )(say, w_qkv, w_out, w_in)


COLOR_COLS = ((0, 384, 768), (768, 1152, 1536), (1536, 1920, 2304))
COLOR_DIMS = ((2, 1, 0), (1, 0, 2), (0, 2, 1))
PIECES = ((0, 1), (1, 1))


def gather_kernel(shard_ref, rows_ref, all_ref, got_ref, send_sem, recv_sem, pair_send, pair_recv, own_sem, row_send, row_recv, row_own):
    me = lax.axis_index("dp")
    core = lax.rem(me, 2)
    place = [lax.div(me, 32), lax.rem(lax.div(me, 8), 4), lax.rem(lax.div(me, 2), 4)]
    stride = (32, 8, 2)

    def neighbour(dim, shift):
        return me + (lax.rem(place[dim] + shift, 4) - place[dim]) * stride[dim]

    partner = me + 1 - 2 * core
    barrier = pltpu.get_barrier_semaphore()

    @pl.loop(1, N_DEV)
    def greet(step):
        pl.semaphore_signal(barrier, inc=1, device_id={"dp": lax.rem(me + step, N_DEV)}, device_id_type=MESH)

    own = pltpu.make_async_copy(shard_ref, all_ref.at[place[0], place[1], place[2], core], own_sem)
    own.start()
    own_rows = pltpu.make_async_copy(rows_ref.at[me], got_ref.at[me], row_own)
    own_rows.start()
    pl.semaphore_wait(barrier, N_DEV - 1)

    @pl.loop(1, N_DEV)
    def give(step):
        peer = lax.rem(me + step, N_DEV)
        pltpu.make_async_remote_copy(
            src_ref=rows_ref.at[peer], dst_ref=got_ref.at[me], send_sem=row_send, recv_sem=row_recv,
            device_id={"dp": peer}, device_id_type=MESH).start()

    sent = []

    def block(piece, color, phase, shift, half):
        start, middle, stop = COLOR_COLS[color]
        if half == 0:
            stop = middle
        if half == 1:
            start = middle
        first, count = PIECES[piece]
        if phase < 0:
            return shard_ref.at[pl.ds(first, count), :, pl.ds(start, stop - start)]
        index = list(place)
        for dim in COLOR_DIMS[color][:phase]:
            index[dim] = slice(None)
        dim = COLOR_DIMS[color][phase]
        index[dim] = lax.rem(place[dim] + shift, 4)
        return all_ref.at[index[0], index[1], index[2], core, pl.ds(first, count), :, pl.ds(start, stop - start)]

    def send(src, dst, sems, number, other):
        copy = pltpu.make_async_remote_copy(
            src_ref=src, dst_ref=dst, send_sem=sems[0].at[number], recv_sem=sems[1].at[number],
            device_id={"dp": other}, device_id_type=MESH)
        copy.start()
        sent.append(copy)

    def arrived(region, sems, number):
        pltpu.make_async_remote_copy(
            src_ref=region, dst_ref=region, send_sem=sems[0].at[number], recv_sem=sems[1].at[number],
            device_id={"dp": partner}, device_id_type=MESH).wait_recv()

    ring, pair = (send_sem, recv_sem), (pair_send, pair_recv)
    todo = [(piece, color) for piece in range(len(PIECES)) for color in range(3)]

    def slot(piece, color, phase, kind):
        return ((piece * 3 + color) * 3 + phase) * 4 + kind

    def pair_slot(piece, color, phase, kind):
        return (piece * 3 + color) * 10 + (0 if phase < 0 else 1 + phase * 3 + kind)

    def begin(piece, color, phase):
        dim = COLOR_DIMS[color][phase]
        dst = block(piece, color, phase, 0, None)
        src = block(piece, color, -1, 0, None) if phase == 0 else dst
        send(src, dst, ring, slot(piece, color, phase, 0), neighbour(dim, 1))
        send(src, dst, ring, slot(piece, color, phase, 1), neighbour(dim, 3))
        if phase == 0:
            send(src, dst, pair, pair_slot(piece, color, -1, 0), partner)

    def forward(piece, color, phase):
        dim = COLOR_DIMS[color][phase]
        for kind, shift in ((0, 3), (1, 1)):
            region = block(piece, color, phase, shift, None)
            arrived(region, ring, slot(piece, color, phase, kind))
            part = block(piece, color, phase, shift, kind)
            send(part, part, ring, slot(piece, color, phase, 2 + kind), neighbour(dim, 1 if kind == 0 else 3))
            send(region, region, pair, pair_slot(piece, color, phase, kind), partner)

    def finish(piece, color, phase):
        for kind in (0, 1):
            arrived(block(piece, color, phase, 2, kind), ring, slot(piece, color, phase, 2 + kind))
        region = block(piece, color, phase, 2, None)
        send(region, region, pair, pair_slot(piece, color, phase, 2), partner)

    for piece, color in todo:
        begin(piece, color, 0)
    own.wait()
    for phase in range(3):
        for piece, color in todo:
            forward(piece, color, phase)
        for piece, color in todo:
            finish(piece, color, phase)
            if phase < 2:
                begin(piece, color, phase + 1)

    for piece, color in todo:
        first, count = PIECES[piece]
        start, _, stop = COLOR_COLS[color]
        tail = (1 - core, pl.ds(first, count), slice(None), pl.ds(start, stop - start))
        arrived(all_ref.at[(place[0], place[1], place[2]) + tail], pair, pair_slot(piece, color, -1, 0))
        for phase in range(3):
            for kind, shift in ((0, 3), (1, 1), (2, 2)):
                index = list(place)
                for dim in COLOR_DIMS[color][:phase]:
                    index[dim] = slice(None)
                dim = COLOR_DIMS[color][phase]
                index[dim] = lax.rem(place[dim] + shift, 4)
                arrived(all_ref.at[tuple(index) + tail], pair, pair_slot(piece, color, phase, kind))
    for copy in sent:
        copy.wait_send()
    rest = pltpu.make_async_remote_copy(
        src_ref=rows_ref.at[pl.ds(0, N_DEV - 1)], dst_ref=got_ref.at[pl.ds(0, N_DEV - 1)], send_sem=row_send, recv_sem=row_recv,
        device_id={"dp": lax.rem(me + 1, N_DEV)}, device_id_type=MESH)
    rest.wait_send()
    rest.wait_recv()
    own_rows.wait()


def gather_near(shard, rows):
    dma = pltpu.SemaphoreType.DMA
    vmem = pl.BlockSpec(memory_space=pltpu.VMEM)
    n_ring, n_pair = len(PIECES) * 36, len(PIECES) * 30
    out, got = pl.pallas_call(
        gather_kernel,
        out_shape=(jax.ShapeDtypeStruct((4, 4, 4, 2) + shard.shape, BF16), jax.ShapeDtypeStruct(rows.shape, BF16)),
        in_specs=[vmem, vmem],
        out_specs=(pl.BlockSpec(memory_space=pl.ANY), vmem),
        scratch_shapes=[dma((n_ring,)), dma((n_ring,)), dma((n_pair,)), dma((n_pair,)), dma, dma, dma, dma],
        compiler_params=pltpu.CompilerParams(collective_id=2, has_side_effects=True),
        cost_estimate=pl.CostEstimate(flops=5 * 10 ** 10, bytes_accessed=10 ** 7, transcendentals=0),
        name="gather",
    )(shard, rows)
    return out.reshape((32, 4) + shard.shape), got.reshape(N_DEV * CAP, D_MODEL)


def exact_dot(a, b):
    return jnp.dot(a, b, precision=lax.Precision.HIGHEST, preferred_element_type=F32)


def plan_requests(tok_ids, seg_ids, shard_rows):
    owner = jnp.where(seg_ids >= 0, tok_ids // shard_rows, -1)
    local = tok_ids % shard_rows
    hot = (owner[:, None] == jnp.arange(N_DEV)[None, :]).astype(BF16)
    earlier = (jnp.arange(N_SLOTS)[:, None] > jnp.arange(N_SLOTS)[None, :]).astype(BF16)
    before = jnp.dot(earlier, hot, preferred_element_type=F32)
    rank = jnp.sum(before * hot.astype(F32), axis=1).astype(jnp.int32)
    counts = jnp.sum(hot.astype(F32), axis=0)
    return owner, local, hot, rank, counts


def ids_to_ask(local, hot, rank, width):
    place = rank[:, None] == jnp.arange(width)[None, :]
    high = jnp.where(place, (local // 32)[:, None], 0).astype(BF16)
    low = jnp.where(place, (local % 32)[:, None], 0).astype(BF16)
    both = lax.dot_general(hot, jnp.concatenate([high, low], axis=1), (((0,), (0,)), ((), ())), preferred_element_type=F32)
    return both[:, :width] * 32.0 + both[:, width:]


def pick_rows(ids, table):
    hot = (ids.reshape(-1, 1) == jnp.arange(table.shape[0]).astype(F32)[None, :]).astype(BF16)
    return jnp.dot(hot, table, preferred_element_type=F32).astype(BF16)


def spilled_rows(asks, wanted, table):
    me = lax.axis_index("dp")
    devs = jnp.arange(N_DEV)
    extra = jnp.maximum(asks - CAP, 0.0)
    sizes = jnp.sum(jnp.where(devs[None, :] == me, extra, 0.0), axis=1)[None, :]
    starts = exact_dot(sizes, (devs[:, None] < devs[None, :]).astype(F32))
    row = jnp.arange(SPILL).astype(F32)[:, None]
    mine = (starts <= row) & (row < starts + sizes)
    rank = jnp.sum(jnp.where(mine, row - starts + CAP, 0.0), axis=1, keepdims=True)
    choice = exact_dot(mine.astype(F32), wanted)
    return pick_rows(jnp.sum(jnp.where(jnp.arange(ASK).astype(F32)[None, :] == rank, choice, 0.0), axis=1), table)


def place_rows(owner, local, hot, rank, asks, got, spilled, table):
    me = lax.axis_index("dp")
    extra = jnp.maximum(asks - CAP, 0.0)
    too_many = (jnp.max(asks) > ASK) | (jnp.max(jnp.sum(extra, axis=0)) > SPILL)
    starts = jnp.sum(jnp.where(jnp.arange(N_DEV)[:, None] < me, extra, 0.0), axis=0)
    base = jnp.sum(hot.astype(F32) * starts[None, :], axis=1).astype(jnp.int32)
    near = jnp.where((owner >= 0) & (rank < CAP), owner * CAP + rank, -1)
    far = jnp.where((owner >= 0) & (rank >= CAP), owner * SPILL + base + rank - CAP, -1)

    def exchanged():
        pick_near = (near[:, None] == jnp.arange(N_DEV * CAP)[None, :]).astype(BF16)
        pick_far = (far[:, None] == jnp.arange(N_DEV * SPILL)[None, :]).astype(BF16)
        return (jnp.dot(pick_near, got, preferred_element_type=F32) + jnp.dot(pick_far, spilled, preferred_element_type=F32)).astype(BF16)

    def by_rounds():
        def one_round(number, rows):
            here = rank - number * CAP
            ids = lax.all_to_all(ids_to_ask(local, hot, here, CAP), "dp", split_axis=0, concat_axis=0, tiled=True)
            sent = pick_rows(ids, table).reshape(N_DEV, CAP, D_MODEL)
            back = lax.all_to_all(sent, "dp", split_axis=0, concat_axis=0, tiled=True).reshape(N_DEV * CAP, D_MODEL)
            slot = jnp.where((owner >= 0) & (here >= 0) & (here < CAP), owner * CAP + here, -1)
            pick = (slot[:, None] == jnp.arange(N_DEV * CAP)[None, :]).astype(BF16)
            return rows + jnp.dot(pick, back, preferred_element_type=F32).astype(BF16)

        rounds = jnp.ceil(jnp.max(asks) / CAP).astype(jnp.int32)
        return lax.fori_loop(0, rounds, one_round, jnp.zeros((N_SLOTS, D_MODEL), BF16))

    return lax.cond(too_many, by_rounds, exchanged)


def rope_tables(positions, theta):
    inv_freq = theta ** (-jnp.arange(0, HEAD_DIM, 2).astype(F32) / HEAD_DIM)
    angles = positions.astype(F32)[:, None] * jnp.tile(inv_freq, 4)[None, :]
    sign = jnp.where(jnp.arange(128) % HEAD_DIM < HEAD_DIM // 2, -1.0, 1.0)
    return jnp.cos(angles), jnp.sin(angles) * sign[None, :]


def key_ranges(seg_ids, positions):
    n_blocks = N_SLOTS // QB
    first = jnp.arange(n_blocks) * QB
    seg_first = seg_ids[::QB]
    lo = jnp.where(seg_first >= 0, first - positions[::QB], first) // QB
    last_seg = jnp.max(seg_ids.reshape(n_blocks, QB), axis=1)
    hi = jnp.sum(((seg_ids >= 0)[None, :] & (seg_ids[None, :] <= last_seg[:, None])).astype(jnp.int32), axis=1)
    span = jnp.maximum(hi - lo * QB, 1)
    kind = jnp.sum((span[:, None] > jnp.array(SPANS)[None, :]).astype(jnp.int32), axis=1)
    return lo.astype(jnp.int32), kind.astype(jnp.int32)


def solution(mesh):
    token_spec = P(("pod", "dp"))
    layer_spec = P(None, "dp", None)
    gain_spec = P(None, "dp")
    in_specs = (token_spec, token_spec, token_spec, P("dp", None), P("dp"), layer_spec, layer_spec, layer_spec, layer_spec, gain_spec, gain_spec, P("dp"))

    def device_program(tok_ids, seg_ids, positions, emb_table, gain_emb, w_qkv, w_out, w_in, w_down, gain_attn, gain_mlp, gain_final):
        owner, local, hot, rank, counts = plan_requests(tok_ids, seg_ids, emb_table.shape[0])
        wanted = ids_to_ask(local, hot, rank, ASK)
        gains = jnp.concatenate([gain_emb[None], gain_attn, gain_mlp, gain_final[None]], axis=0).astype(F32).reshape(1, -1)
        n_gain = gains.shape[1]
        tail = jnp.concatenate([wanted, jnp.broadcast_to(gains, (N_DEV, n_gain)), jnp.zeros((N_DEV, 128 - ASK - n_gain), F32)], axis=1)
        say = jnp.stack([jnp.broadcast_to(counts[None, :], (N_DEV, N_DEV)), tail], axis=1)
        heard, quarters = meet(say, w_qkv, w_out, w_in)
        asks, asked = heard[:, 0, :], heard[:, 1, :ASK]
        shard = jnp.concatenate([quarters.transpose(1, 0, 2, 3).reshape(N_LAYERS, 16, 1536), w_down], axis=2)
        far_weights = lax.all_gather(shard[2:].reshape(1, 2, 16, LAYER_COLS), "dp", axis=0, tiled=True).reshape(32, 4, 2, 16, LAYER_COLS)
        spill = spilled_rows(asks, asked, emb_table).reshape(SPILL, 2, 256).transpose(1, 0, 2)
        rows = pick_rows(asked[:, :CAP], emb_table).reshape(N_DEV, CAP, D_MODEL)
        near_weights, got = gather_near(jnp.concatenate([shard[:2], spill], axis=2), rows)
        spilled = near_weights[:, :, :, :, LAYER_COLS:].transpose(0, 1, 3, 2, 4).reshape(N_DEV * SPILL, D_MODEL)
        hidden = place_rows(owner, local, hot, rank, asks, got, spilled, emb_table)
        gains = heard[:, 1, ASK:ASK + n_gain].reshape(N_DEV, n_gain // 4, 4).transpose(1, 0, 2).reshape(n_gain // 4, D_MODEL)
        seg_key = jnp.where(seg_ids >= 0, seg_ids, -2)
        segc, segr = seg_ids[:, None], seg_key[None, :]
        segs = jnp.pad(segr, ((0, 0), (WINDOW_HALF, WINDOW_HALF)), constant_values=-2)
        lo, kind = key_ranges(seg_ids, positions)
        tables = (rope_tables(positions, THETA_GLOBAL), rope_tables(positions, THETA_LOCAL))
        for layer in range(N_LAYERS):
            cos_t, sin_t = tables[int(layer % 3 != 0)]
            hidden = run_layer(layer, lo, kind, hidden, segc, segr, segs, cos_t, sin_t, gains, near_weights if layer < 2 else far_weights)
        return hidden

    return jax.shard_map(device_program, mesh=mesh, in_specs=in_specs, out_specs=P(("pod", "dp"), None), check_vma=False)
```

```python
import functools

import jax
import jax.numpy as jnp
from jax import lax
from jax.experimental import pallas as pl
from jax.experimental.pallas import tpu as pltpu
from jax.sharding import PartitionSpec as P

D_MODEL = 512
FF_DIM = 2048
N_LAYERS = 4
N_SLOTS = 1024
HEAD_DIM = 64
N_PAIRS = 4
WINDOW_HALF = 64
DOC_SLOTS = 32
LN_EPS = 1e-5
THETA_GLOBAL = 160000.0
THETA_LOCAL = 10000.0
NEG_BIG = -1e30
LOG2_E = 1.4426950408889634
N_DEV = 128
ASK = 80
CAP = 16
SPILL = 16
MESH = pl.DeviceIdType.MESH
QB = 128
ROWS = 256
LAYER_COLS = 2048
NEAR_COLS = LAYER_COLS + 512
SPANS = (256, 384, 512, 640, 768, 896, 1024)
COST = pl.CostEstimate(flops=20000000000, bytes_accessed=10000000, transcendentals=10000000)
F32 = jnp.float32
BF16 = jnp.bfloat16


def ln_rows(as_float, gain_row):
    centered = as_float - jnp.mean(as_float, axis=-1, keepdims=True)
    variance = jnp.mean(centered * centered, axis=-1, keepdims=True)
    return centered * lax.rsqrt(variance + LN_EPS) * gain_row


def layer_kernel(layer, *refs):
    is_first, is_last, is_local = layer == 0, layer == N_LAYERS - 1, layer % 3 != 0
    refs = list(refs)
    lo_ref, kind_ref, x_ref, segc_ref, cos_ref, sin_ref, gain_ref, w_ref = refs[:8]
    refs = refs[8:]
    if is_first:
        near_ref, far_ref, late_ref = refs[:3]
        refs = refs[3:]
    if is_last:
        segr_ref = refs.pop(0)
    out_ref, w_s, q_s, k_s, v_s, c_s, z_s, sems = refs[:8]
    extra_s = refs[8] if len(refs) > 8 else None
    x_s = extra_s if is_last else out_ref
    index = 1 if is_last else 0
    ranges = [(0, 384), (384, 128), (512, 1024), (1536, 512)]
    copies = [
        pltpu.make_async_copy(w_ref.at[:, :, index, :, pl.ds(start, size)], w_s.at[:, :, :, pl.ds(start, size)], sems.at[number])
        for number, (start, size) in enumerate(ranges)
    ]
    if is_first:
        spill = pltpu.make_async_copy(w_ref.at[:, :, 0, :, pl.ds(LAYER_COLS, 512)], extra_s, sems.at[4])
        spill.start()
    copies[0].start()
    pad = WINDOW_HALF
    lane = lax.broadcasted_iota(jnp.int32, (1, 128), 1)
    lane_doc = lane % HEAD_DIM
    low_half = lane_doc < HEAD_DIM // 2
    first_head = lane < HEAD_DIM
    if is_local:
        for half in range(2):
            fill = jnp.broadcast_to(jnp.where(first_head == (half == 0), 0.0, NEG_BIG), (pad, 128)).astype(BF16)
            for pair in range(N_PAIRS):
                k_s[2 * pair + half, pl.ds(0, pad), :] = fill
                k_s[2 * pair + half, pl.ds(pad + N_SLOTS, pad), :] = fill
        zeros = jnp.zeros((pad, 128), BF16)
        for pair in range(N_PAIRS):
            v_s[pair, pl.ds(0, pad), :] = zeros
            v_s[pair, pl.ds(pad + N_SLOTS, pad), :] = zeros
        qi = lax.broadcasted_iota(jnp.int32, (QB, 2 * QB), 0)
        kj = lax.broadcasted_iota(jnp.int32, (QB, 2 * QB), 1)
        extra_s[...] = jnp.where((kj >= qi) & (kj - qi <= 2 * WINDOW_HALF), 0.0, NEG_BIG)

    def weight(quarter, start, size):
        return w_s[:, quarter, :, start:start + size].reshape(D_MODEL, size)

    if is_first:
        spill.wait()
    copies[0].wait()
    for copy in copies[1:]:
        copy.start()

    @pl.loop(0, N_SLOTS // ROWS)
    def qkv_rows(block):
        rows = pl.ds(pl.multiple_of(block * ROWS, ROWS), ROWS)
        prows = pl.ds(pl.multiple_of(block * ROWS + pad, pad), ROWS)
        if is_first:
            number = lax.broadcasted_iota(jnp.int32, (1, N_DEV * CAP), 1)
            near = jnp.where(near_ref[rows, :] == number, 1.0, 0.0).astype(BF16)
            far = jnp.where(far_ref[rows, :] == number, 1.0, 0.0).astype(BF16)
            x = jnp.dot(near, x_ref[...], preferred_element_type=F32)
            x = x + jnp.dot(far, extra_s[...].reshape(N_DEV * SPILL, D_MODEL), preferred_element_type=F32)
            x = x + late_ref[rows, :].astype(F32)
            u = ln_rows(x, gain_ref[0:1, :]).astype(BF16)
            x_s[rows, :] = u
        else:
            u = ln_rows(x_ref[rows, :].astype(F32), gain_ref[layer:layer + 1, :]).astype(BF16)
        cos_t, sin_t = cos_ref[rows, :], sin_ref[rows, :]
        same = lane_doc == segc_ref[rows, :]
        q_doc = jnp.where(same, 1.0, 0.0)
        k_doc = jnp.where(same, 0.0, NEG_BIG)

        def rope(h):
            h = h.astype(F32)
            turned = jnp.where(low_half, pltpu.roll(h, 96, 1), pltpu.roll(h, 32, 1))
            return h * cos_t + turned * sin_t

        for pair in range(N_PAIRS):
            qkv = jnp.dot(u, weight(pair, 0, 384), preferred_element_type=F32).astype(BF16)
            q = rope(qkv[:, :128])
            k = rope(qkv[:, 128:256])
            q_s[2 * pair, rows, :] = jnp.where(first_head, q, q_doc).astype(BF16)
            q_s[2 * pair + 1, rows, :] = jnp.where(first_head, q_doc, q).astype(BF16)
            k_s[2 * pair, prows, :] = jnp.where(first_head, k, k_doc).astype(BF16)
            k_s[2 * pair + 1, prows, :] = jnp.where(first_head, k_doc, k).astype(BF16)
            v_s[pair, prows, :] = qkv[:, 256:]

    def attend(pair, qrows, krows):
        halves = []
        for half in range(2):
            q, k = q_s[2 * pair + half, qrows, :], k_s[2 * pair + half, krows, :]
            s = lax.dot_general(q, k, (((1,), (1,)), ((), ())), preferred_element_type=F32)
            if is_local:
                s = s + extra_s[...]
            e = jnp.exp2((s - jnp.max(s, axis=1, keepdims=True)) * (LOG2_E * HEAD_DIM ** -0.5))
            p = (e * (1.0 / jnp.sum(e, axis=1, keepdims=True))).astype(BF16)
            halves.append(jnp.dot(p, v_s[pair, krows, :], preferred_element_type=F32))
        c_s[pair, qrows, :] = jnp.where(first_head, halves[0], halves[1]).astype(BF16)

    @pl.loop(0, N_SLOTS // QB, unroll=2 if is_local else 1)
    def query_block(block):
        qrows = pl.ds(pl.multiple_of(block * QB, QB), QB)
        if is_local:
            for pair in range(N_PAIRS):
                attend(pair, qrows, pl.ds(pl.multiple_of(block * QB, QB), 2 * QB))
            return
        kind = kind_ref[block]
        for number, span in enumerate(SPANS):
            @pl.when(kind == number)
            def run():
                k0 = jnp.minimum(lo_ref[block] * QB, N_SLOTS - span)
                krows = pl.ds(pl.multiple_of(k0 + pad, pad), span)
                if span <= 512:
                    for pair in range(N_PAIRS):
                        attend(pair, qrows, krows)
                else:
                    @pl.loop(0, N_PAIRS, unroll=2)
                    def one_pair(pair):
                        attend(pair, qrows, krows)

    for copy in copies[1:]:
        copy.wait()

    @pl.loop(0, N_SLOTS // ROWS)
    def mlp_rows(block):
        rows = pl.ds(pl.multiple_of(block * ROWS, ROWS), ROWS)
        w_out = jnp.concatenate([weight(quarter, 384, 128) for quarter in range(4)], axis=1)
        context = jnp.concatenate([c_s[pair, rows, :] for pair in range(N_PAIRS)], axis=1)
        attn = jnp.dot(context, w_out, preferred_element_type=F32)
        x = x_s[rows, :] if is_first else x_ref[rows, :]
        hidden = (x.astype(F32) + attn).astype(BF16)
        m = ln_rows(hidden.astype(F32), gain_ref[4 + layer:5 + layer, :]).astype(BF16)
        for j in range(8):
            quarter, start = j // 2, (j % 2) * 256
            a = jnp.dot(m, weight(quarter, 512 + start, 256), preferred_element_type=F32)
            b = jnp.dot(m, weight(quarter, 1024 + start, 256), preferred_element_type=F32)
            gelu = 0.5 * a * (1.0 + lax.erf(a * (0.5 ** 0.5)))
            z_s[:, j * 256:(j + 1) * 256] = (gelu * b).astype(BF16)
        down = jnp.dot(z_s[...], w_s[:, :, :, 1536:].reshape(FF_DIM, D_MODEL), preferred_element_type=F32)
        x_s[rows, :] = (hidden.astype(F32) + down).astype(BF16)

    if is_last:
        docs = lax.broadcasted_iota(jnp.int32, (DOC_SLOTS, N_SLOTS), 0)
        member = (docs == segr_ref[...]).astype(F32)
        f = ln_rows(x_s[...].astype(F32), gain_ref[8:9, :])
        sums = jnp.dot(member, f, precision=lax.Precision.HIGHEST, preferred_element_type=F32)
        out_ref[...] = sums / jnp.maximum(jnp.sum(member, axis=1, keepdims=True), 1.0)


def run_layer(layer, lo, kind, x, segc, cos_t, sin_t, gains, weights, more):
    is_first, is_last = layer == 0, layer == N_LAYERS - 1
    vmem = pl.BlockSpec(memory_space=pltpu.VMEM)
    smem = pl.BlockSpec(memory_space=pltpu.SMEM)
    scratch = [
        pltpu.VMEM((32, 4, 16, LAYER_COLS), BF16),
        pltpu.VMEM((2 * N_PAIRS, N_SLOTS, 128), BF16), pltpu.VMEM((2 * N_PAIRS, N_SLOTS + 128, 128), BF16),
        pltpu.VMEM((N_PAIRS, N_SLOTS + 128, 128), BF16), pltpu.VMEM((N_PAIRS, N_SLOTS, 128), BF16), pltpu.VMEM((ROWS, FF_DIM), BF16),
        pltpu.SemaphoreType.DMA((5,)),
    ]
    out_shape = jax.ShapeDtypeStruct((N_SLOTS, D_MODEL), BF16)
    if is_first:
        scratch.append(pltpu.VMEM((32, 4, 16, 512), BF16))
    elif is_last:
        out_shape = jax.ShapeDtypeStruct((DOC_SLOTS, D_MODEL), F32)
        scratch.append(pltpu.VMEM((N_SLOTS, D_MODEL), BF16))
    else:
        scratch.append(pltpu.VMEM((QB, 2 * QB), F32))
    return pl.pallas_call(
        functools.partial(layer_kernel, layer),
        out_shape=out_shape,
        in_specs=[smem, smem] + [vmem] * 5 + [pl.BlockSpec(memory_space=pl.ANY)] + [vmem] * len(more),
        out_specs=vmem,
        scratch_shapes=scratch,
        compiler_params=pltpu.CompilerParams(vmem_limit_bytes=48 * 2 ** 20),
        cost_estimate=COST,
        name=f"layer_{layer}",
    )(lo, kind, x, segc, cos_t, sin_t, gains, weights, *more)


def meet_kernel(say_ref, qkv_ref, out_ref, in_ref, heard_ref, quart_ref, send_sem, recv_sem, own_sem, w_send, w_recv, w_own):
    me = lax.axis_index("dp")
    mine = lax.rem(me, 4)
    barrier = pltpu.get_barrier_semaphore()

    @pl.loop(1, N_DEV)
    def greet(step):
        pl.semaphore_signal(barrier, inc=1, device_id={"dp": lax.rem(me + step, N_DEV)}, device_id_type=MESH)

    own = [pltpu.make_async_copy(say_ref.at[me], heard_ref.at[me], own_sem)]

    def pieces(quarter, slot):
        out = []
        for part in range(3):
            cols = pl.ds(pl.multiple_of(part * 512 + quarter * 128, 128), 128)
            out.append((qkv_ref.at[:, :, cols], quart_ref.at[slot, :, :, pl.ds(part * 128, 128)]))
        out.append((out_ref.at[:, :, pl.ds(pl.multiple_of(quarter * 128, 128), 128)], quart_ref.at[slot, :, :, pl.ds(384, 128)]))
        for part in range(2):
            cols = pl.ds(pl.multiple_of(part * 2048 + quarter * 512, 512), 512)
            out.append((in_ref.at[:, :, cols], quart_ref.at[slot, :, :, pl.ds(512 + part * 512, 512)]))
        return out

    own += [pltpu.make_async_copy(src, dst, w_own.at[index]) for index, (src, dst) in enumerate(pieces(mine, mine))]
    for copy in own:
        copy.start()
    pl.semaphore_wait(barrier, N_DEV - 1)

    quarters = []
    for step in range(1, 4):
        quarter = lax.rem(mine + step, 4)
        for index, (src, dst) in enumerate(pieces(quarter, mine)):
            number = (step - 1) * 6 + index
            quarters.append(pltpu.make_async_remote_copy(
                src_ref=src, dst_ref=dst, send_sem=w_send.at[number], recv_sem=w_recv.at[number],
                device_id={"dp": me - mine + quarter}, device_id_type=MESH))
    for copy in quarters:
        copy.start()

    @pl.loop(1, N_DEV)
    def tell(step):
        peer = lax.rem(me + step, N_DEV)
        pltpu.make_async_remote_copy(
            src_ref=say_ref.at[peer], dst_ref=heard_ref.at[me], send_sem=send_sem, recv_sem=recv_sem,
            device_id={"dp": peer}, device_id_type=MESH).start()

    rest = pltpu.make_async_remote_copy(
        src_ref=say_ref.at[pl.ds(0, N_DEV - 1)], dst_ref=heard_ref.at[pl.ds(0, N_DEV - 1)], send_sem=send_sem, recv_sem=recv_sem,
        device_id={"dp": lax.rem(me + 1, N_DEV)}, device_id_type=MESH)
    rest.wait_send()
    rest.wait_recv()
    for copy in own + quarters:
        copy.wait()


def meet(say, w_qkv, w_out, w_in):
    vmem = pl.BlockSpec(memory_space=pltpu.VMEM)
    dma = pltpu.SemaphoreType.DMA
    return pl.pallas_call(
        meet_kernel,
        out_shape=(jax.ShapeDtypeStruct(say.shape, F32), jax.ShapeDtypeStruct((4, N_LAYERS, 4, 1536), BF16)),
        in_specs=[vmem] * 4,
        out_specs=(vmem, vmem),
        scratch_shapes=[dma, dma, dma, dma((18,)), dma((18,)), dma((6,))],
        compiler_params=pltpu.CompilerParams(collective_id=1, has_side_effects=True),
        cost_estimate=COST,
        name="meet",
    )(say, w_qkv, w_out, w_in)


COLOR_COLS = ((0, 512, 896), (896, 1408, 1792), (1792, 2176, 2560))
COLOR_DIMS = ((2, 1, 0), (1, 0, 2), (0, 2, 1))
PIECES = ((0, 1),)


def gather_kernel(shard_ref, rows_ref, all_ref, got_ref, send_sem, recv_sem, pair_send, pair_recv, own_sem, row_send, row_recv, row_own):
    me = lax.axis_index("dp")
    core = lax.rem(me, 2)
    place = [lax.div(me, 32), lax.rem(lax.div(me, 8), 4), lax.rem(lax.div(me, 2), 4)]
    stride = (32, 8, 2)

    def neighbour(dim, shift):
        return me + (lax.rem(place[dim] + shift, 4) - place[dim]) * stride[dim]

    partner = me + 1 - 2 * core
    barrier = pltpu.get_barrier_semaphore()

    @pl.loop(1, N_DEV)
    def greet(step):
        pl.semaphore_signal(barrier, inc=1, device_id={"dp": lax.rem(me + step, N_DEV)}, device_id_type=MESH)

    own = pltpu.make_async_copy(shard_ref, all_ref.at[place[0], place[1], place[2], core], own_sem)
    own.start()
    own_rows = pltpu.make_async_copy(rows_ref.at[me], got_ref.at[me], row_own)
    own_rows.start()
    pl.semaphore_wait(barrier, N_DEV - 1)

    @pl.loop(1, N_DEV)
    def give(step):
        peer = lax.rem(me + step, N_DEV)
        pltpu.make_async_remote_copy(
            src_ref=rows_ref.at[peer], dst_ref=got_ref.at[me], send_sem=row_send, recv_sem=row_recv,
            device_id={"dp": peer}, device_id_type=MESH).start()

    sent = []

    def block(piece, color, phase, shift, half):
        start, middle, stop = COLOR_COLS[color]
        if half == 0:
            stop = middle
        if half == 1:
            start = middle
        first, count = PIECES[piece]
        if phase < 0:
            return shard_ref.at[pl.ds(first, count), :, pl.ds(start, stop - start)]
        index = list(place)
        for dim in COLOR_DIMS[color][:phase]:
            index[dim] = slice(None)
        dim = COLOR_DIMS[color][phase]
        index[dim] = lax.rem(place[dim] + shift, 4)
        return all_ref.at[index[0], index[1], index[2], core, pl.ds(first, count), :, pl.ds(start, stop - start)]

    def send(src, dst, sems, number, other):
        copy = pltpu.make_async_remote_copy(
            src_ref=src, dst_ref=dst, send_sem=sems[0].at[number], recv_sem=sems[1].at[number],
            device_id={"dp": other}, device_id_type=MESH)
        copy.start()
        sent.append(copy)

    def arrived(region, sems, number):
        pltpu.make_async_remote_copy(
            src_ref=region, dst_ref=region, send_sem=sems[0].at[number], recv_sem=sems[1].at[number],
            device_id={"dp": partner}, device_id_type=MESH).wait_recv()

    ring, pair = (send_sem, recv_sem), (pair_send, pair_recv)
    todo = [(piece, color) for piece in range(len(PIECES)) for color in range(3)]

    def slot(piece, color, phase, kind):
        return ((piece * 3 + color) * 3 + phase) * 4 + kind

    def pair_slot(piece, color, phase, kind):
        return (piece * 3 + color) * 10 + (0 if phase < 0 else 1 + phase * 3 + kind)

    def begin(piece, color, phase):
        dim = COLOR_DIMS[color][phase]
        dst = block(piece, color, phase, 0, None)
        src = block(piece, color, -1, 0, None) if phase == 0 else dst
        send(src, dst, ring, slot(piece, color, phase, 0), neighbour(dim, 1))
        send(src, dst, ring, slot(piece, color, phase, 1), neighbour(dim, 3))
        if phase == 0:
            send(src, dst, pair, pair_slot(piece, color, -1, 0), partner)

    def forward(piece, color, phase):
        dim = COLOR_DIMS[color][phase]
        for kind, shift in ((0, 3), (1, 1)):
            region = block(piece, color, phase, shift, None)
            arrived(region, ring, slot(piece, color, phase, kind))
            part = block(piece, color, phase, shift, kind)
            send(part, part, ring, slot(piece, color, phase, 2 + kind), neighbour(dim, 1 if kind == 0 else 3))
            send(region, region, pair, pair_slot(piece, color, phase, kind), partner)

    def finish(piece, color, phase):
        for kind in (0, 1):
            arrived(block(piece, color, phase, 2, kind), ring, slot(piece, color, phase, 2 + kind))
        region = block(piece, color, phase, 2, None)
        send(region, region, pair, pair_slot(piece, color, phase, 2), partner)

    for piece, color in todo:
        begin(piece, color, 0)
    own.wait()
    for phase in range(3):
        for piece, color in todo:
            forward(piece, color, phase)
        for piece, color in todo:
            finish(piece, color, phase)
            if phase < 2:
                begin(piece, color, phase + 1)

    for piece, color in todo:
        first, count = PIECES[piece]
        start, _, stop = COLOR_COLS[color]
        tail = (1 - core, pl.ds(first, count), slice(None), pl.ds(start, stop - start))
        arrived(all_ref.at[(place[0], place[1], place[2]) + tail], pair, pair_slot(piece, color, -1, 0))
        for phase in range(3):
            for kind, shift in ((0, 3), (1, 1), (2, 2)):
                index = list(place)
                for dim in COLOR_DIMS[color][:phase]:
                    index[dim] = slice(None)
                dim = COLOR_DIMS[color][phase]
                index[dim] = lax.rem(place[dim] + shift, 4)
                arrived(all_ref.at[tuple(index) + tail], pair, pair_slot(piece, color, phase, kind))
    for copy in sent:
        copy.wait_send()
    rest = pltpu.make_async_remote_copy(
        src_ref=rows_ref.at[pl.ds(0, N_DEV - 1)], dst_ref=got_ref.at[pl.ds(0, N_DEV - 1)], send_sem=row_send, recv_sem=row_recv,
        device_id={"dp": lax.rem(me + 1, N_DEV)}, device_id_type=MESH)
    rest.wait_send()
    rest.wait_recv()
    own_rows.wait()


def gather_near(shard, rows):
    dma = pltpu.SemaphoreType.DMA
    vmem = pl.BlockSpec(memory_space=pltpu.VMEM)
    n_ring, n_pair = len(PIECES) * 36, len(PIECES) * 30
    out, got = pl.pallas_call(
        gather_kernel,
        out_shape=(jax.ShapeDtypeStruct((4, 4, 4, 2) + shard.shape, BF16), jax.ShapeDtypeStruct(rows.shape, BF16)),
        in_specs=[vmem, vmem],
        out_specs=(pl.BlockSpec(memory_space=pl.ANY), vmem),
        scratch_shapes=[dma((n_ring,)), dma((n_ring,)), dma((n_pair,)), dma((n_pair,)), dma, dma, dma, dma],
        compiler_params=pltpu.CompilerParams(collective_id=2, has_side_effects=True),
        cost_estimate=COST,
        name="gather",
    )(shard, rows)
    return out.reshape((32, 4) + shard.shape), got.reshape(N_DEV * CAP, D_MODEL)


def exact_dot(a, b):
    return jnp.dot(a, b, precision=lax.Precision.HIGHEST, preferred_element_type=F32)


def plan_requests(tok_ids, seg_ids, shard_rows):
    owner = jnp.where(seg_ids >= 0, tok_ids // shard_rows, -1)
    local = tok_ids % shard_rows
    hot = (owner[:, None] == jnp.arange(N_DEV)[None, :]).astype(BF16)
    earlier = (jnp.arange(N_SLOTS)[:, None] > jnp.arange(N_SLOTS)[None, :]).astype(BF16)
    before = jnp.dot(earlier, hot, preferred_element_type=F32)
    rank = jnp.sum(before * hot.astype(F32), axis=1).astype(jnp.int32)
    counts = jnp.sum(hot.astype(F32), axis=0)
    return owner, local, hot, rank, counts


def ids_to_ask(local, hot, rank, width):
    place = rank[:, None] == jnp.arange(width)[None, :]
    high = jnp.where(place, (local // 32)[:, None], 0).astype(BF16)
    low = jnp.where(place, (local % 32)[:, None], 0).astype(BF16)
    both = lax.dot_general(hot, jnp.concatenate([high, low], axis=1), (((0,), (0,)), ((), ())), preferred_element_type=F32)
    return both[:, :width] * 32.0 + both[:, width:]


def pick_rows(ids, table):
    hot = (ids.reshape(-1, 1) == jnp.arange(table.shape[0]).astype(F32)[None, :]).astype(BF16)
    return jnp.dot(hot, table, preferred_element_type=F32).astype(BF16)


def spilled_rows(asks, wanted, table):
    me = lax.axis_index("dp")
    devs = jnp.arange(N_DEV)
    extra = jnp.maximum(asks - CAP, 0.0)
    sizes = jnp.sum(jnp.where(devs[None, :] == me, extra, 0.0), axis=1)[None, :]
    starts = exact_dot(sizes, (devs[:, None] < devs[None, :]).astype(F32))
    row = jnp.arange(SPILL).astype(F32)[:, None]
    mine = (starts <= row) & (row < starts + sizes)
    rank = jnp.sum(jnp.where(mine, row - starts + CAP, 0.0), axis=1, keepdims=True)
    choice = exact_dot(mine.astype(F32), wanted)
    return pick_rows(jnp.sum(jnp.where(jnp.arange(ASK).astype(F32)[None, :] == rank, choice, 0.0), axis=1), table)


def place_rows(owner, local, hot, rank, asks, table):
    me = lax.axis_index("dp")
    extra = jnp.maximum(asks - CAP, 0.0)
    too_many = (jnp.max(asks) > ASK) | (jnp.max(jnp.sum(extra, axis=0)) > SPILL)
    starts = jnp.sum(jnp.where(jnp.arange(N_DEV)[:, None] < me, extra, 0.0), axis=0)
    base = jnp.sum(hot.astype(F32) * starts[None, :], axis=1).astype(jnp.int32)
    near = jnp.where((owner >= 0) & (rank < CAP), owner * CAP + rank, -1)
    far = jnp.where((owner >= 0) & (rank >= CAP), owner * SPILL + base + rank - CAP, -1)

    def by_rounds():
        def one_round(number, rows):
            here = rank - number * CAP
            ids = lax.all_to_all(ids_to_ask(local, hot, here, CAP), "dp", split_axis=0, concat_axis=0, tiled=True)
            sent = pick_rows(ids, table).reshape(N_DEV, CAP, D_MODEL)
            back = lax.all_to_all(sent, "dp", split_axis=0, concat_axis=0, tiled=True).reshape(N_DEV * CAP, D_MODEL)
            slot = jnp.where((owner >= 0) & (here >= 0) & (here < CAP), owner * CAP + here, -1)
            pick = (slot[:, None] == jnp.arange(N_DEV * CAP)[None, :]).astype(BF16)
            return rows + jnp.dot(pick, back, preferred_element_type=F32).astype(BF16)

        rounds = jnp.ceil(jnp.max(asks) / CAP).astype(jnp.int32)
        return lax.fori_loop(0, rounds, one_round, none())

    def none():
        return jnp.zeros((N_SLOTS, D_MODEL), BF16)

    near = jnp.where(too_many, -1, near)
    far = jnp.where(too_many, -1, far)
    return near[:, None], far[:, None], lax.cond(too_many, by_rounds, none)


def rope_tables(positions, theta):
    inv_freq = theta ** (-jnp.arange(0, HEAD_DIM, 2).astype(F32) / HEAD_DIM)
    angles = positions.astype(F32)[:, None] * jnp.tile(inv_freq, 4)[None, :]
    sign = jnp.where(jnp.arange(128) % HEAD_DIM < HEAD_DIM // 2, -1.0, 1.0)
    return jnp.cos(angles), jnp.sin(angles) * sign[None, :]


def key_ranges(seg_ids, positions):
    n_blocks = N_SLOTS // QB
    first = jnp.arange(n_blocks) * QB
    seg_first = seg_ids[::QB]
    lo = jnp.where(seg_first >= 0, first - positions[::QB], first) // QB
    last_seg = jnp.max(seg_ids.reshape(n_blocks, QB), axis=1)
    hi = jnp.sum(((seg_ids >= 0)[None, :] & (seg_ids[None, :] <= last_seg[:, None])).astype(jnp.int32), axis=1)
    span = jnp.maximum(hi - lo * QB, 1)
    kind = jnp.sum((span[:, None] > jnp.array(SPANS)[None, :]).astype(jnp.int32), axis=1)
    return lo.astype(jnp.int32), kind.astype(jnp.int32)


def solution(mesh):
    token_spec = P(("pod", "dp"))
    layer_spec = P(None, "dp", None)
    gain_spec = P(None, "dp")
    in_specs = (token_spec, token_spec, token_spec, P("dp", None), P("dp"), layer_spec, layer_spec, layer_spec, layer_spec, gain_spec, gain_spec, P("dp"))

    def device_program(tok_ids, seg_ids, positions, emb_table, gain_emb, w_qkv, w_out, w_in, w_down, gain_attn, gain_mlp, gain_final):
        owner, local, hot, rank, counts = plan_requests(tok_ids, seg_ids, emb_table.shape[0])
        wanted = ids_to_ask(local, hot, rank, ASK)
        gains = jnp.concatenate([gain_emb[None], gain_attn, gain_mlp, gain_final[None]], axis=0).astype(F32).reshape(1, -1)
        n_gain = gains.shape[1]
        tail = jnp.concatenate([wanted, jnp.broadcast_to(gains, (N_DEV, n_gain)), jnp.zeros((N_DEV, 128 - ASK - n_gain), F32)], axis=1)
        say = jnp.stack([jnp.broadcast_to(counts[None, :], (N_DEV, N_DEV)), tail], axis=1)
        heard, quarters = meet(say, w_qkv, w_out, w_in)
        asks, asked = heard[:, 0, :], heard[:, 1, :ASK]
        shard = jnp.concatenate([quarters.transpose(1, 0, 2, 3).reshape(N_LAYERS, 16, 1536), w_down], axis=2)
        next_weights, last_weights = (
            lax.all_gather(part[None], "dp", axis=0, tiled=True).reshape((32, 4) + part.shape) for part in (shard[1:2], shard[2:]))
        spill = spilled_rows(asks, asked, emb_table)[None]
        rows = pick_rows(asked[:, :CAP], emb_table).reshape(N_DEV, CAP, D_MODEL)
        near_weights, hidden = gather_near(jnp.concatenate([shard[:1], spill], axis=2), rows)
        near, far, late = place_rows(owner, local, hot, rank, asks, emb_table)
        gains = heard[:, 1, ASK:ASK + n_gain].reshape(N_DEV, n_gain // 4, 4).transpose(1, 0, 2).reshape(n_gain // 4, D_MODEL)
        segc = seg_ids[:, None]
        lo, kind = key_ranges(seg_ids, positions)
        tables = (rope_tables(positions, THETA_GLOBAL), rope_tables(positions, THETA_LOCAL))
        for layer in range(N_LAYERS):
            cos_t, sin_t = tables[int(layer % 3 != 0)]
            more = [near, far, late] if layer == 0 else [seg_ids[None, :]] if layer == N_LAYERS - 1 else []
            hidden = run_layer(layer, lo, kind, hidden, segc, cos_t, sin_t, gains, (near_weights, next_weights, last_weights, last_weights)[layer], more)
        return hidden

    return jax.shard_map(device_program, mesh=mesh, in_specs=in_specs, out_specs=P(("pod", "dp"), None), check_vma=False)
```

```python
import functools

import jax
import jax.numpy as jnp
from jax import lax
from jax.experimental import pallas as pl
from jax.experimental.pallas import tpu as pltpu
from jax.sharding import PartitionSpec as P

D_MODEL = 512
FF_DIM = 2048
N_LAYERS = 4
N_SLOTS = 1024
HEAD_DIM = 64
N_PAIRS = 4
WINDOW_HALF = 64
DOC_SLOTS = 32
LN_EPS = 1e-5
THETA_GLOBAL = 160000.0
THETA_LOCAL = 10000.0
NEG_BIG = -1e30
LOG2_E = 1.4426950408889634
N_DEV = 128
ASK = 80
CAP = 16
SPILL = 16
MESH = pl.DeviceIdType.MESH
QB = 128
GLOBAL_QB = 256
VMEM_BYTES = 50331648
ROWS = 256
LAYER_COLS = 2048
NEAR_COLS = LAYER_COLS + 512
SPANS = (256, 384, 512, 640, 768, 896, 1024)
COST = pl.CostEstimate(flops=20000000000, bytes_accessed=10000000, transcendentals=10000000)
F32 = jnp.float32
BF16 = jnp.bfloat16


def ln_rows(as_float, gain_row):
    centered = as_float - jnp.mean(as_float, axis=-1, keepdims=True)
    variance = jnp.mean(centered * centered, axis=-1, keepdims=True)
    return centered * lax.rsqrt(variance + LN_EPS) * gain_row


def layer_kernel(layer, *refs):
    is_first, is_last, is_local = layer == 0, layer == N_LAYERS - 1, layer % 3 != 0
    refs = list(refs)
    lo_ref, kind_ref, x_ref, segc_ref, cos_ref, sin_ref, gain_ref, w_ref = refs[:8]
    refs = refs[8:]
    if is_first:
        near_ref, far_ref, late_ref = refs[:3]
        refs = refs[3:]
    if is_last:
        segr_ref = refs.pop(0)
    out_ref, w_s, q_s, k_s, v_s, c_s, z_s, sems = refs[:8]
    extra_s = refs[8] if len(refs) > 8 else None
    x_s = extra_s if is_last else out_ref
    index = 1 if is_last else 0
    ranges = [(0, 384), (384, 128), (512, 1024), (1536, 512)]
    copies = [
        pltpu.make_async_copy(w_ref.at[:, :, index, :, pl.ds(start, size)], w_s.at[:, :, :, pl.ds(start, size)], sems.at[number])
        for number, (start, size) in enumerate(ranges)
    ]
    if is_first:
        spill = pltpu.make_async_copy(w_ref.at[:, :, 0, :, pl.ds(LAYER_COLS, 512)], extra_s, sems.at[4])
        spill.start()
    copies[0].start()
    pad = WINDOW_HALF
    lane = lax.broadcasted_iota(jnp.int32, (1, 128), 1)
    lane_doc = lane % HEAD_DIM
    low_half = lane_doc < HEAD_DIM // 2
    first_head = lane < HEAD_DIM
    if is_local:
        for half in range(2):
            fill = jnp.broadcast_to(jnp.where(first_head == (half == 0), 0.0, NEG_BIG), (pad, 128)).astype(BF16)
            for pair in range(N_PAIRS):
                k_s[2 * pair + half, pl.ds(0, pad), :] = fill
                k_s[2 * pair + half, pl.ds(pad + N_SLOTS, pad), :] = fill
        zeros = jnp.zeros((pad, 128), BF16)
        for pair in range(N_PAIRS):
            v_s[pair, pl.ds(0, pad), :] = zeros
            v_s[pair, pl.ds(pad + N_SLOTS, pad), :] = zeros
        qi = lax.broadcasted_iota(jnp.int32, (QB, 2 * QB), 0)
        kj = lax.broadcasted_iota(jnp.int32, (QB, 2 * QB), 1)
        extra_s[...] = jnp.where((kj >= qi) & (kj - qi <= 2 * WINDOW_HALF), 0.0, NEG_BIG)

    def weight(quarter, start, size):
        return w_s[:, quarter, :, start:start + size].reshape(D_MODEL, size)

    if is_first:
        spill.wait()
    copies[0].wait()
    for copy in copies[1:]:
        copy.start()

    @pl.loop(0, N_SLOTS // ROWS)
    def qkv_rows(block):
        rows = pl.ds(pl.multiple_of(block * ROWS, ROWS), ROWS)
        prows = pl.ds(pl.multiple_of(block * ROWS + pad, pad), ROWS)
        if is_first:
            number = lax.broadcasted_iota(jnp.int32, (1, N_DEV * CAP), 1)
            near = jnp.where(near_ref[rows, :] == number, 1.0, 0.0).astype(BF16)
            far = jnp.where(far_ref[rows, :] == number, 1.0, 0.0).astype(BF16)
            x = jnp.dot(near, x_ref[...], preferred_element_type=F32)
            x = x + jnp.dot(far, extra_s[...].reshape(N_DEV * SPILL, D_MODEL), preferred_element_type=F32)
            x = x + late_ref[rows, :].astype(F32)
            u = ln_rows(x, gain_ref[0:1, :]).astype(BF16)
            x_s[rows, :] = u
        else:
            u = ln_rows(x_ref[rows, :].astype(F32), gain_ref[layer:layer + 1, :]).astype(BF16)
        cos_t, sin_t = cos_ref[rows, :], sin_ref[rows, :]
        same = lane_doc == segc_ref[rows, :]
        q_doc = jnp.where(same, 1.0, 0.0)
        k_doc = jnp.where(same, 0.0, NEG_BIG)

        def rope(h):
            h = h.astype(F32)
            turned = jnp.where(low_half, pltpu.roll(h, 96, 1), pltpu.roll(h, 32, 1))
            return h * cos_t + turned * sin_t

        for pair in range(N_PAIRS):
            qkv = jnp.dot(u, weight(pair, 0, 384), preferred_element_type=F32).astype(BF16)
            q = rope(qkv[:, :128])
            k = rope(qkv[:, 128:256])
            q_s[2 * pair, rows, :] = jnp.where(first_head, q, q_doc).astype(BF16)
            q_s[2 * pair + 1, rows, :] = jnp.where(first_head, q_doc, q).astype(BF16)
            k_s[2 * pair, prows, :] = jnp.where(first_head, k, k_doc).astype(BF16)
            k_s[2 * pair + 1, prows, :] = jnp.where(first_head, k_doc, k).astype(BF16)
            v_s[pair, prows, :] = qkv[:, 256:]

    def attend(pair, qrows, krows):
        halves = []
        for half in range(2):
            q, k = q_s[2 * pair + half, qrows, :], k_s[2 * pair + half, krows, :]
            s = lax.dot_general(q, k, (((1,), (1,)), ((), ())), preferred_element_type=F32)
            if is_local:
                s = s + extra_s[...]
            e = jnp.exp2((s - jnp.max(s, axis=1, keepdims=True)) * (LOG2_E * HEAD_DIM ** -0.5))
            p = (e * (1.0 / jnp.sum(e, axis=1, keepdims=True))).astype(BF16)
            halves.append(jnp.dot(p, v_s[pair, krows, :], preferred_element_type=F32))
        c_s[pair, qrows, :] = jnp.where(first_head, halves[0], halves[1]).astype(BF16)

    if is_local:
        @pl.loop(0, N_SLOTS // QB, unroll=2)
        def local_block(block):
            start = pl.multiple_of(block * QB, QB)
            for pair in range(N_PAIRS):
                attend(pair, pl.ds(start, QB), pl.ds(start, 2 * QB))
    else:
        @pl.loop(0, N_SLOTS // GLOBAL_QB)
        def global_block(block):
            qrows = pl.ds(pl.multiple_of(block * GLOBAL_QB, GLOBAL_QB), GLOBAL_QB)
            kind = kind_ref[block]
            for number, span in enumerate(SPANS):
                @pl.when(kind == number)
                def run():
                    k0 = jnp.minimum(lo_ref[block] * QB, N_SLOTS - span)
                    krows = pl.ds(pl.multiple_of(k0 + pad, pad), span)

                    @pl.loop(0, N_PAIRS, unroll=2 if span <= 384 else 1)
                    def one_pair(pair):
                        attend(pair, qrows, krows)

    for copy in copies[1:]:
        copy.wait()

    @pl.loop(0, N_SLOTS // ROWS)
    def mlp_rows(block):
        rows = pl.ds(pl.multiple_of(block * ROWS, ROWS), ROWS)
        w_out = jnp.concatenate([weight(quarter, 384, 128) for quarter in range(4)], axis=1)
        context = jnp.concatenate([c_s[pair, rows, :] for pair in range(N_PAIRS)], axis=1)
        attn = jnp.dot(context, w_out, preferred_element_type=F32)
        x = x_s[rows, :] if is_first else x_ref[rows, :]
        hidden = (x.astype(F32) + attn).astype(BF16)
        m = ln_rows(hidden.astype(F32), gain_ref[4 + layer:5 + layer, :]).astype(BF16)
        for j in range(8):
            quarter, start = j // 2, (j % 2) * 256
            a = jnp.dot(m, weight(quarter, 512 + start, 256), preferred_element_type=F32)
            b = jnp.dot(m, weight(quarter, 1024 + start, 256), preferred_element_type=F32)
            gelu = 0.5 * a * (1.0 + lax.erf(a * (0.5 ** 0.5)))
            z_s[:, j * 256:(j + 1) * 256] = (gelu * b).astype(BF16)
        down = jnp.dot(z_s[...], w_s[:, :, :, 1536:].reshape(FF_DIM, D_MODEL), preferred_element_type=F32)
        x_s[rows, :] = (hidden.astype(F32) + down).astype(BF16)

    if is_last:
        docs = lax.broadcasted_iota(jnp.int32, (DOC_SLOTS, N_SLOTS), 0)
        member = (docs == segr_ref[...]).astype(F32)
        f = ln_rows(x_s[...].astype(F32), gain_ref[8:9, :])
        sums = jnp.dot(member, f, precision=lax.Precision.HIGHEST, preferred_element_type=F32)
        out_ref[...] = sums / jnp.maximum(jnp.sum(member, axis=1, keepdims=True), 1.0)


def run_layer(layer, lo, kind, x, segc, cos_t, sin_t, gains, weights, more):
    is_first, is_last = layer == 0, layer == N_LAYERS - 1
    vmem = pl.BlockSpec(memory_space=pltpu.VMEM)
    smem = pl.BlockSpec(memory_space=pltpu.SMEM)
    scratch = [
        pltpu.VMEM((32, 4, 16, LAYER_COLS), BF16),
        pltpu.VMEM((2 * N_PAIRS, N_SLOTS, 128), BF16), pltpu.VMEM((2 * N_PAIRS, N_SLOTS + 128, 128), BF16),
        pltpu.VMEM((N_PAIRS, N_SLOTS + 128, 128), BF16), pltpu.VMEM((N_PAIRS, N_SLOTS, 128), BF16), pltpu.VMEM((ROWS, FF_DIM), BF16),
        pltpu.SemaphoreType.DMA((5,)),
    ]
    out_shape = jax.ShapeDtypeStruct((N_SLOTS, D_MODEL), BF16)
    if is_first:
        scratch.append(pltpu.VMEM((32, 4, 16, 512), BF16))
    elif is_last:
        out_shape = jax.ShapeDtypeStruct((DOC_SLOTS, D_MODEL), F32)
        scratch.append(pltpu.VMEM((N_SLOTS, D_MODEL), BF16))
    else:
        scratch.append(pltpu.VMEM((QB, 2 * QB), F32))
    return pl.pallas_call(
        functools.partial(layer_kernel, layer),
        out_shape=out_shape,
        in_specs=[smem, smem] + [vmem] * 5 + [pl.BlockSpec(memory_space=pltpu.HBM)] + [vmem] * len(more),
        out_specs=vmem,
        scratch_shapes=scratch,
        compiler_params=pltpu.CompilerParams(vmem_limit_bytes=VMEM_BYTES),
        cost_estimate=COST,
        name=f"layer_{layer}",
    )(lo, kind, x, segc, cos_t, sin_t, gains, weights, *more)


def meet_kernel(say_ref, qkv_ref, out_ref, in_ref, heard_ref, quart_ref, send_sem, recv_sem, own_sem, w_send, w_recv, w_own):
    me = lax.axis_index("dp")
    mine = lax.rem(me, 4)
    barrier = pltpu.get_barrier_semaphore()

    @pl.loop(1, N_DEV)
    def greet(step):
        pl.semaphore_signal(barrier, inc=1, device_id={"dp": lax.rem(me + step, N_DEV)}, device_id_type=MESH)

    own = [pltpu.make_async_copy(say_ref.at[me], heard_ref.at[me], own_sem)]

    def pieces(quarter, slot):
        out = []
        for part in range(3):
            cols = pl.ds(pl.multiple_of(part * 512 + quarter * 128, 128), 128)
            out.append((qkv_ref.at[:, :, cols], quart_ref.at[slot, :, :, pl.ds(part * 128, 128)]))
        out.append((out_ref.at[:, :, pl.ds(pl.multiple_of(quarter * 128, 128), 128)], quart_ref.at[slot, :, :, pl.ds(384, 128)]))
        for part in range(2):
            cols = pl.ds(pl.multiple_of(part * 2048 + quarter * 512, 512), 512)
            out.append((in_ref.at[:, :, cols], quart_ref.at[slot, :, :, pl.ds(512 + part * 512, 512)]))
        return out

    own += [pltpu.make_async_copy(src, dst, w_own.at[index]) for index, (src, dst) in enumerate(pieces(mine, mine))]
    for copy in own:
        copy.start()
    pl.semaphore_wait(barrier, N_DEV - 1)

    quarters = []
    for step in range(1, 4):
        quarter = lax.rem(mine + step, 4)
        for index, (src, dst) in enumerate(pieces(quarter, mine)):
            number = (step - 1) * 6 + index
            quarters.append(pltpu.make_async_remote_copy(
                src_ref=src, dst_ref=dst, send_sem=w_send.at[number], recv_sem=w_recv.at[number],
                device_id={"dp": me - mine + quarter}, device_id_type=MESH))
    for copy in quarters:
        copy.start()

    @pl.loop(1, N_DEV)
    def tell(step):
        peer = lax.rem(me + step, N_DEV)
        pltpu.make_async_remote_copy(
            src_ref=say_ref.at[peer], dst_ref=heard_ref.at[me], send_sem=send_sem, recv_sem=recv_sem,
            device_id={"dp": peer}, device_id_type=MESH).start()

    rest = pltpu.make_async_remote_copy(
        src_ref=say_ref.at[pl.ds(0, N_DEV - 1)], dst_ref=heard_ref.at[pl.ds(0, N_DEV - 1)], send_sem=send_sem, recv_sem=recv_sem,
        device_id={"dp": lax.rem(me + 1, N_DEV)}, device_id_type=MESH)
    rest.wait_send()
    rest.wait_recv()
    for copy in own + quarters:
        copy.wait()


def meet(say, w_qkv, w_out, w_in):
    vmem = pl.BlockSpec(memory_space=pltpu.VMEM)
    dma = pltpu.SemaphoreType.DMA
    return pl.pallas_call(
        meet_kernel,
        out_shape=(jax.ShapeDtypeStruct(say.shape, F32), jax.ShapeDtypeStruct((4, N_LAYERS, 4, 1536), BF16)),
        in_specs=[vmem] * 4,
        out_specs=(vmem, vmem),
        scratch_shapes=[dma, dma, dma, dma((18,)), dma((18,)), dma((6,))],
        compiler_params=pltpu.CompilerParams(collective_id=1, has_side_effects=True),
        cost_estimate=COST,
        name="meet",
    )(say, w_qkv, w_out, w_in)


COLOR_COLS = ((0, 512, 896), (896, 1408, 1792), (1792, 2176, 2560))
COLOR_DIMS = ((2, 1, 0), (1, 0, 2), (0, 2, 1))
PIECES = ((0, 1),)


def gather_kernel(shard_ref, rows_ref, all_ref, got_ref, send_sem, recv_sem, pair_send, pair_recv, own_sem, row_send, row_recv, row_own):
    me = lax.axis_index("dp")
    core = lax.rem(me, 2)
    place = [lax.div(me, 32), lax.rem(lax.div(me, 8), 4), lax.rem(lax.div(me, 2), 4)]
    stride = (32, 8, 2)

    def neighbour(dim, shift):
        return me + (lax.rem(place[dim] + shift, 4) - place[dim]) * stride[dim]

    partner = me + 1 - 2 * core
    barrier = pltpu.get_barrier_semaphore()

    @pl.loop(1, N_DEV)
    def greet(step):
        pl.semaphore_signal(barrier, inc=1, device_id={"dp": lax.rem(me + step, N_DEV)}, device_id_type=MESH)

    own = pltpu.make_async_copy(shard_ref, all_ref.at[place[0], place[1], place[2], core], own_sem)
    own.start()
    own_rows = pltpu.make_async_copy(rows_ref.at[me], got_ref.at[me], row_own)
    own_rows.start()
    pl.semaphore_wait(barrier, N_DEV - 1)

    def give(part):
        @pl.loop(max(part * 22, 1), min(part * 22 + 22, N_DEV))
        def to_peer(step):
            peer = lax.rem(me + step, N_DEV)
            pltpu.make_async_remote_copy(
                src_ref=rows_ref.at[peer], dst_ref=got_ref.at[me], send_sem=row_send, recv_sem=row_recv,
                device_id={"dp": peer}, device_id_type=MESH).start()

    sent = []

    def block(piece, color, phase, shift, half):
        start, middle, stop = COLOR_COLS[color]
        if half == 0:
            stop = middle
        if half == 1:
            start = middle
        first, count = PIECES[piece]
        if phase < 0:
            return shard_ref.at[pl.ds(first, count), :, pl.ds(start, stop - start)]
        index = list(place)
        for dim in COLOR_DIMS[color][:phase]:
            index[dim] = slice(None)
        dim = COLOR_DIMS[color][phase]
        index[dim] = lax.rem(place[dim] + shift, 4)
        return all_ref.at[index[0], index[1], index[2], core, pl.ds(first, count), :, pl.ds(start, stop - start)]

    def send(src, dst, sems, number, other):
        copy = pltpu.make_async_remote_copy(
            src_ref=src, dst_ref=dst, send_sem=sems[0].at[number], recv_sem=sems[1].at[number],
            device_id={"dp": other}, device_id_type=MESH)
        copy.start()
        sent.append(copy)

    def arrived(region, sems, number):
        pltpu.make_async_remote_copy(
            src_ref=region, dst_ref=region, send_sem=sems[0].at[number], recv_sem=sems[1].at[number],
            device_id={"dp": partner}, device_id_type=MESH).wait_recv()

    ring, pair = (send_sem, recv_sem), (pair_send, pair_recv)
    todo = [(piece, color) for piece in range(len(PIECES)) for color in range(3)]

    def slot(piece, color, phase, kind):
        return ((piece * 3 + color) * 3 + phase) * 4 + kind

    def pair_slot(piece, color, phase, kind):
        return (piece * 3 + color) * 10 + (0 if phase < 0 else 1 + phase * 3 + kind)

    def begin(piece, color, phase):
        dim = COLOR_DIMS[color][phase]
        dst = block(piece, color, phase, 0, None)
        src = block(piece, color, -1, 0, None) if phase == 0 else dst
        send(src, dst, ring, slot(piece, color, phase, 0), neighbour(dim, 1))
        send(src, dst, ring, slot(piece, color, phase, 1), neighbour(dim, 3))
        if phase == 0:
            send(src, dst, pair, pair_slot(piece, color, -1, 0), partner)

    def forward(piece, color, phase):
        dim = COLOR_DIMS[color][phase]
        for kind, shift in ((0, 3), (1, 1)):
            region = block(piece, color, phase, shift, None)
            arrived(region, ring, slot(piece, color, phase, kind))
            part = block(piece, color, phase, shift, kind)
            send(part, part, ring, slot(piece, color, phase, 2 + kind), neighbour(dim, 1 if kind == 0 else 3))
            send(region, region, pair, pair_slot(piece, color, phase, kind), partner)

    def finish(piece, color, phase):
        for kind in (0, 1):
            arrived(block(piece, color, phase, 2, kind), ring, slot(piece, color, phase, 2 + kind))
        region = block(piece, color, phase, 2, None)
        send(region, region, pair, pair_slot(piece, color, phase, 2), partner)

    for piece, color in todo:
        begin(piece, color, 0)
    give(0)
    own.wait()
    for phase in range(3):
        for piece, color in todo:
            forward(piece, color, phase)
        give(1 + 2 * phase)
        for piece, color in todo:
            finish(piece, color, phase)
            if phase < 2:
                begin(piece, color, phase + 1)
        if phase < 2:
            give(2 + 2 * phase)

    for piece, color in todo:
        first, count = PIECES[piece]
        start, _, stop = COLOR_COLS[color]
        tail = (1 - core, pl.ds(first, count), slice(None), pl.ds(start, stop - start))
        arrived(all_ref.at[(place[0], place[1], place[2]) + tail], pair, pair_slot(piece, color, -1, 0))
        for phase in range(3):
            for kind, shift in ((0, 3), (1, 1), (2, 2)):
                index = list(place)
                for dim in COLOR_DIMS[color][:phase]:
                    index[dim] = slice(None)
                dim = COLOR_DIMS[color][phase]
                index[dim] = lax.rem(place[dim] + shift, 4)
                arrived(all_ref.at[tuple(index) + tail], pair, pair_slot(piece, color, phase, kind))
    for copy in sent:
        copy.wait_send()
    rest = pltpu.make_async_remote_copy(
        src_ref=rows_ref.at[pl.ds(0, N_DEV - 1)], dst_ref=got_ref.at[pl.ds(0, N_DEV - 1)], send_sem=row_send, recv_sem=row_recv,
        device_id={"dp": lax.rem(me + 1, N_DEV)}, device_id_type=MESH)
    rest.wait_send()
    rest.wait_recv()
    own_rows.wait()


def gather_near(shard, rows):
    dma = pltpu.SemaphoreType.DMA
    vmem = pl.BlockSpec(memory_space=pltpu.VMEM)
    n_ring, n_pair = len(PIECES) * 36, len(PIECES) * 30
    out, got = pl.pallas_call(
        gather_kernel,
        out_shape=(jax.ShapeDtypeStruct((4, 4, 4, 2) + shard.shape, BF16), jax.ShapeDtypeStruct(rows.shape, BF16)),
        in_specs=[vmem, vmem],
        out_specs=(pl.BlockSpec(memory_space=pltpu.HBM), vmem),
        scratch_shapes=[dma((n_ring,)), dma((n_ring,)), dma((n_pair,)), dma((n_pair,)), dma, dma, dma, dma],
        compiler_params=pltpu.CompilerParams(collective_id=2, has_side_effects=True),
        cost_estimate=COST,
        name="gather",
    )(shard, rows)
    return out.reshape((32, 4) + shard.shape), got.reshape(N_DEV * CAP, D_MODEL)


def exact_dot(a, b):
    return jnp.dot(a, b, precision=lax.Precision.HIGHEST, preferred_element_type=F32)


def plan_requests(tok_ids, seg_ids, shard_rows):
    owner = jnp.where(seg_ids >= 0, tok_ids // shard_rows, -1)
    local = tok_ids % shard_rows
    hot = (owner[:, None] == jnp.arange(N_DEV)[None, :]).astype(BF16)
    earlier = (jnp.arange(N_SLOTS)[:, None] > jnp.arange(N_SLOTS)[None, :]).astype(BF16)
    before = jnp.dot(earlier, hot, preferred_element_type=F32)
    rank = jnp.sum(before * hot.astype(F32), axis=1).astype(jnp.int32)
    counts = jnp.sum(hot.astype(F32), axis=0)
    return owner, local, hot, rank, counts


def ids_to_ask(local, hot, rank, width):
    place = rank[:, None] == jnp.arange(width)[None, :]
    high = jnp.where(place, (local // 32)[:, None], 0).astype(BF16)
    low = jnp.where(place, (local % 32)[:, None], 0).astype(BF16)
    both = lax.dot_general(hot, jnp.concatenate([high, low], axis=1), (((0,), (0,)), ((), ())), preferred_element_type=F32)
    return both[:, :width] * 32.0 + both[:, width:]


def pick_rows(ids, table):
    hot = (ids.reshape(-1, 1) == jnp.arange(table.shape[0]).astype(F32)[None, :]).astype(BF16)
    return jnp.dot(hot, table, preferred_element_type=F32).astype(BF16)


def spilled_rows(asks, wanted, table):
    me = lax.axis_index("dp")
    devs = jnp.arange(N_DEV)
    extra = jnp.maximum(asks - CAP, 0.0)
    sizes = jnp.sum(jnp.where(devs[None, :] == me, extra, 0.0), axis=1)[None, :]
    starts = exact_dot(sizes, (devs[:, None] < devs[None, :]).astype(F32))
    row = jnp.arange(SPILL).astype(F32)[:, None]
    mine = (starts <= row) & (row < starts + sizes)
    rank = jnp.sum(jnp.where(mine, row - starts + CAP, 0.0), axis=1, keepdims=True)
    choice = exact_dot(mine.astype(F32), wanted)
    return pick_rows(jnp.sum(jnp.where(jnp.arange(ASK).astype(F32)[None, :] == rank, choice, 0.0), axis=1), table)


def place_rows(owner, local, hot, rank, asks, table):
    me = lax.axis_index("dp")
    extra = jnp.maximum(asks - CAP, 0.0)
    too_many = (jnp.max(asks) > ASK) | (jnp.max(jnp.sum(extra, axis=0)) > SPILL)
    starts = jnp.sum(jnp.where(jnp.arange(N_DEV)[:, None] < me, extra, 0.0), axis=0)
    base = jnp.sum(hot.astype(F32) * starts[None, :], axis=1).astype(jnp.int32)
    near = jnp.where((owner >= 0) & (rank < CAP), owner * CAP + rank, -1)
    far = jnp.where((owner >= 0) & (rank >= CAP), owner * SPILL + base + rank - CAP, -1)

    def by_rounds():
        def one_round(number, rows):
            here = rank - number * CAP
            ids = lax.all_to_all(ids_to_ask(local, hot, here, CAP), "dp", split_axis=0, concat_axis=0, tiled=True)
            sent = pick_rows(ids, table).reshape(N_DEV, CAP, D_MODEL)
            back = lax.all_to_all(sent, "dp", split_axis=0, concat_axis=0, tiled=True).reshape(N_DEV * CAP, D_MODEL)
            slot = jnp.where((owner >= 0) & (here >= 0) & (here < CAP), owner * CAP + here, -1)
            pick = (slot[:, None] == jnp.arange(N_DEV * CAP)[None, :]).astype(BF16)
            return rows + jnp.dot(pick, back, preferred_element_type=F32).astype(BF16)

        rounds = jnp.ceil(jnp.max(asks) / CAP).astype(jnp.int32)
        return lax.fori_loop(0, rounds, one_round, none())

    def none():
        return jnp.zeros((N_SLOTS, D_MODEL), BF16)

    near = jnp.where(too_many, -1, near)
    far = jnp.where(too_many, -1, far)
    return near[:, None], far[:, None], lax.cond(too_many, by_rounds, none)


def rope_tables(positions, theta):
    inv_freq = theta ** (-jnp.arange(0, HEAD_DIM, 2).astype(F32) / HEAD_DIM)
    angles = positions.astype(F32)[:, None] * jnp.tile(inv_freq, 4)[None, :]
    sign = jnp.where(jnp.arange(128) % HEAD_DIM < HEAD_DIM // 2, -1.0, 1.0)
    return jnp.cos(angles), jnp.sin(angles) * sign[None, :]


def key_ranges(seg_ids, positions):
    n_blocks = N_SLOTS // GLOBAL_QB
    first = jnp.arange(n_blocks) * GLOBAL_QB
    seg_first = seg_ids[::GLOBAL_QB]
    lo = jnp.where(seg_first >= 0, first - positions[::GLOBAL_QB], first) // QB
    last_seg = jnp.max(seg_ids.reshape(n_blocks, GLOBAL_QB), axis=1)
    hi = jnp.sum(((seg_ids >= 0)[None, :] & (seg_ids[None, :] <= last_seg[:, None])).astype(jnp.int32), axis=1)
    span = jnp.maximum(hi - lo * QB, 1)
    kind = jnp.sum((span[:, None] > jnp.array(SPANS)[None, :]).astype(jnp.int32), axis=1)
    return lo.astype(jnp.int32), kind.astype(jnp.int32)


def solution(mesh):
    token_spec = P(("pod", "dp"))
    layer_spec = P(None, "dp", None)
    gain_spec = P(None, "dp")
    in_specs = (token_spec, token_spec, token_spec, P("dp", None), P("dp"), layer_spec, layer_spec, layer_spec, layer_spec, gain_spec, gain_spec, P("dp"))

    def device_program(tok_ids, seg_ids, positions, emb_table, gain_emb, w_qkv, w_out, w_in, w_down, gain_attn, gain_mlp, gain_final):
        owner, local, hot, rank, counts = plan_requests(tok_ids, seg_ids, emb_table.shape[0])
        wanted = ids_to_ask(local, hot, rank, ASK)
        gains = jnp.concatenate([gain_emb[None], gain_attn, gain_mlp, gain_final[None]], axis=0).astype(F32).reshape(1, -1)
        n_gain = gains.shape[1]
        tail = jnp.concatenate([wanted, jnp.broadcast_to(gains, (N_DEV, n_gain)), jnp.zeros((N_DEV, 128 - ASK - n_gain), F32)], axis=1)
        say = jnp.stack([jnp.broadcast_to(counts[None, :], (N_DEV, N_DEV)), tail], axis=1)
        heard, quarters = meet(say, w_qkv, w_out, w_in)
        asks, asked = heard[:, 0, :], heard[:, 1, :ASK]
        shard = jnp.concatenate([quarters.transpose(1, 0, 2, 3).reshape(N_LAYERS, 16, 1536), w_down], axis=2)
        next_weights, last_weights = (
            lax.all_gather(part[None], "dp", axis=0, tiled=True).reshape((32, 4) + part.shape) for part in (shard[1:2], shard[2:]))
        spill = spilled_rows(asks, asked, emb_table)[None]
        rows = pick_rows(asked[:, :CAP], emb_table).reshape(N_DEV, CAP, D_MODEL)
        near_weights, hidden = gather_near(jnp.concatenate([shard[:1], spill], axis=2), rows)
        near, far, late = place_rows(owner, local, hot, rank, asks, emb_table)
        gains = heard[:, 1, ASK:ASK + n_gain].reshape(N_DEV, n_gain // 4, 4).transpose(1, 0, 2).reshape(n_gain // 4, D_MODEL)
        segc = seg_ids[:, None]
        lo, kind = key_ranges(seg_ids, positions)
        tables = (rope_tables(positions, THETA_GLOBAL), rope_tables(positions, THETA_LOCAL))
        for layer in range(N_LAYERS):
            cos_t, sin_t = tables[int(layer % 3 != 0)]
            more = [near, far, late] if layer == 0 else [seg_ids[None, :]] if layer == N_LAYERS - 1 else []
            hidden = run_layer(layer, lo, kind, hidden, segc, cos_t, sin_t, gains, (near_weights, next_weights, last_weights, last_weights)[layer], more)
        return hidden

    return jax.shard_map(device_program, mesh=mesh, in_specs=in_specs, out_specs=P(("pod", "dp"), None), check_vma=False)
```

```python
import functools

import jax
import jax.numpy as jnp
from jax import lax
from jax.experimental import pallas as pl
from jax.experimental.pallas import tpu as pltpu
from jax.sharding import PartitionSpec as P

D_MODEL = 512
FF_DIM = 2048
N_LAYERS = 4
N_SLOTS = 1024
HEAD_DIM = 64
N_PAIRS = 4
WINDOW_HALF = 64
DOC_SLOTS = 32
LN_EPS = 1e-5
THETA_GLOBAL = 160000.0
THETA_LOCAL = 10000.0
NEG_BIG = -1e30
LOG2_E = 1.4426950408889634
N_DEV = 128
ASK = 80
CAP = 16
SPILL = 16
MESH = pl.DeviceIdType.MESH
QB = 128
GLOBAL_QB = 256
VMEM_BYTES = 50331648
ROWS = 256
LAYER_COLS = 2048
NEAR_COLS = LAYER_COLS + 512
SPANS = (256, 384, 512, 640, 768, 896, 1024)
COST = pl.CostEstimate(flops=20000000000, bytes_accessed=10000000, transcendentals=10000000)
F32 = jnp.float32
BF16 = jnp.bfloat16


def ln_rows(as_float, gain_row):
    centered = as_float - jnp.mean(as_float, axis=-1, keepdims=True)
    variance = jnp.mean(centered * centered, axis=-1, keepdims=True)
    return centered * lax.rsqrt(variance + LN_EPS) * gain_row


def layer_kernel(layer, *refs):
    is_first, is_last, is_local = layer == 0, layer == N_LAYERS - 1, layer % 3 != 0
    refs = list(refs)
    lo_ref, kind_ref, x_ref, segc_ref, cos_ref, sin_ref, gain_ref, w_ref = refs[:8]
    refs = refs[8:]
    if is_first:
        near_ref, far_ref, late_ref = refs[:3]
        refs = refs[3:]
    if is_last:
        segr_ref = refs.pop(0)
    out_ref, w_s, q_s, k_s, v_s, c_s, z_s, sems = refs[:8]
    extra_s = refs[8] if len(refs) > 8 else None
    x_s = extra_s if is_last else out_ref
    index = 0 if is_first else layer - 1
    ranges = [(0, 384), (384, 128), (512, 1024), (1536, 512)]
    copies = [
        pltpu.make_async_copy(w_ref.at[:, :, index, :, pl.ds(start, size)], w_s.at[:, :, :, pl.ds(start, size)], sems.at[number])
        for number, (start, size) in enumerate(ranges)
    ]
    if is_first:
        spill = pltpu.make_async_copy(w_ref.at[:, :, 0, :, pl.ds(LAYER_COLS, 512)], extra_s, sems.at[4])
        spill.start()
    copies[0].start()
    pad = WINDOW_HALF
    lane = lax.broadcasted_iota(jnp.int32, (1, 128), 1)
    lane_doc = lane % HEAD_DIM
    low_half = lane_doc < HEAD_DIM // 2
    first_head = lane < HEAD_DIM
    if is_local:
        for half in range(2):
            fill = jnp.broadcast_to(jnp.where(first_head == (half == 0), 0.0, NEG_BIG), (pad, 128)).astype(BF16)
            for pair in range(N_PAIRS):
                k_s[2 * pair + half, pl.ds(0, pad), :] = fill
                k_s[2 * pair + half, pl.ds(pad + N_SLOTS, pad), :] = fill
        zeros = jnp.zeros((pad, 128), BF16)
        for pair in range(N_PAIRS):
            v_s[pair, pl.ds(0, pad), :] = zeros
            v_s[pair, pl.ds(pad + N_SLOTS, pad), :] = zeros
        qi = lax.broadcasted_iota(jnp.int32, (QB, 2 * QB), 0)
        kj = lax.broadcasted_iota(jnp.int32, (QB, 2 * QB), 1)
        extra_s[...] = jnp.where((kj >= qi) & (kj - qi <= 2 * WINDOW_HALF), 0.0, NEG_BIG)

    def weight(quarter, start, size):
        return w_s[:, quarter, :, start:start + size].reshape(D_MODEL, size)

    if is_first:
        spill.wait()
    copies[0].wait()
    for copy in copies[1:]:
        copy.start()

    @pl.loop(0, N_SLOTS // ROWS)
    def qkv_rows(block):
        rows = pl.ds(pl.multiple_of(block * ROWS, ROWS), ROWS)
        prows = pl.ds(pl.multiple_of(block * ROWS + pad, pad), ROWS)
        if is_first:
            number = lax.broadcasted_iota(jnp.int32, (1, N_DEV * CAP), 1)
            near = jnp.where(near_ref[rows, :] == number, 1.0, 0.0).astype(BF16)
            far = jnp.where(far_ref[rows, :] == number, 1.0, 0.0).astype(BF16)
            x = jnp.dot(near, x_ref[...], preferred_element_type=F32)
            x = x + jnp.dot(far, extra_s[...].reshape(N_DEV * SPILL, D_MODEL), preferred_element_type=F32)
            x = x + late_ref[rows, :].astype(F32)
            u = ln_rows(x, gain_ref[0:1, :]).astype(BF16)
            x_s[rows, :] = u
        else:
            u = ln_rows(x_ref[rows, :].astype(F32), gain_ref[layer:layer + 1, :]).astype(BF16)
        cos_t, sin_t = cos_ref[rows, :], sin_ref[rows, :]
        same = lane_doc == segc_ref[rows, :]
        q_doc = jnp.where(same, 1.0, 0.0)
        k_doc = jnp.where(same, 0.0, NEG_BIG)

        def rope(h):
            h = h.astype(F32)
            turned = jnp.where(low_half, pltpu.roll(h, 96, 1), pltpu.roll(h, 32, 1))
            return h * cos_t + turned * sin_t

        for pair in range(N_PAIRS):
            qkv = jnp.dot(u, weight(pair, 0, 384), preferred_element_type=F32).astype(BF16)
            q = rope(qkv[:, :128])
            k = rope(qkv[:, 128:256])
            q_s[2 * pair, rows, :] = jnp.where(first_head, q, q_doc).astype(BF16)
            q_s[2 * pair + 1, rows, :] = jnp.where(first_head, q_doc, q).astype(BF16)
            k_s[2 * pair, prows, :] = jnp.where(first_head, k, k_doc).astype(BF16)
            k_s[2 * pair + 1, prows, :] = jnp.where(first_head, k_doc, k).astype(BF16)
            v_s[pair, prows, :] = qkv[:, 256:]

    def attend(pair, qrows, krows):
        halves = []
        for half in range(2):
            q, k = q_s[2 * pair + half, qrows, :], k_s[2 * pair + half, krows, :]
            s = lax.dot_general(q, k, (((1,), (1,)), ((), ())), preferred_element_type=F32)
            if is_local:
                s = s + extra_s[...]
            e = jnp.exp2((s - jnp.max(s, axis=1, keepdims=True)) * (LOG2_E * HEAD_DIM ** -0.5))
            p = (e * (1.0 / jnp.sum(e, axis=1, keepdims=True))).astype(BF16)
            halves.append(jnp.dot(p, v_s[pair, krows, :], preferred_element_type=F32))
        c_s[pair, qrows, :] = jnp.where(first_head, halves[0], halves[1]).astype(BF16)

    if is_local:
        @pl.loop(0, N_SLOTS // QB, unroll=2)
        def local_block(block):
            start = pl.multiple_of(block * QB, QB)
            for pair in range(N_PAIRS):
                attend(pair, pl.ds(start, QB), pl.ds(start, 2 * QB))
    else:
        @pl.loop(0, N_SLOTS // GLOBAL_QB)
        def global_block(block):
            qrows = pl.ds(pl.multiple_of(block * GLOBAL_QB, GLOBAL_QB), GLOBAL_QB)
            kind = kind_ref[block]
            for number, span in enumerate(SPANS):
                @pl.when(kind == number)
                def run():
                    k0 = jnp.minimum(lo_ref[block] * QB, N_SLOTS - span)
                    krows = pl.ds(pl.multiple_of(k0 + pad, pad), span)

                    @pl.loop(0, N_PAIRS)
                    def one_pair(pair):
                        attend(pair, qrows, krows)

    for copy in copies[1:]:
        copy.wait()

    @pl.loop(0, N_SLOTS // ROWS)
    def mlp_rows(block):
        rows = pl.ds(pl.multiple_of(block * ROWS, ROWS), ROWS)
        w_out = jnp.concatenate([weight(quarter, 384, 128) for quarter in range(4)], axis=1)
        context = jnp.concatenate([c_s[pair, rows, :] for pair in range(N_PAIRS)], axis=1)
        attn = jnp.dot(context, w_out, preferred_element_type=F32)
        x = x_s[rows, :] if is_first else x_ref[rows, :]
        hidden = (x.astype(F32) + attn).astype(BF16)
        m = ln_rows(hidden.astype(F32), gain_ref[4 + layer:5 + layer, :]).astype(BF16)
        for j in range(8):
            quarter, start = j // 2, (j % 2) * 256
            a = jnp.dot(m, weight(quarter, 512 + start, 256), preferred_element_type=F32)
            b = jnp.dot(m, weight(quarter, 1024 + start, 256), preferred_element_type=F32)
            gelu = 0.5 * a * (1.0 + lax.erf(a * (0.5 ** 0.5)))
            z_s[:, j * 256:(j + 1) * 256] = (gelu * b).astype(BF16)
        down = jnp.dot(z_s[...], w_s[:, :, :, 1536:].reshape(FF_DIM, D_MODEL), preferred_element_type=F32)
        x_s[rows, :] = (hidden.astype(F32) + down).astype(BF16)

    if is_last:
        docs = lax.broadcasted_iota(jnp.int32, (DOC_SLOTS, N_SLOTS), 0)
        member = (docs == segr_ref[...]).astype(F32)
        f = ln_rows(x_s[...].astype(F32), gain_ref[8:9, :])
        sums = jnp.dot(member, f, precision=lax.Precision.HIGHEST, preferred_element_type=F32)
        out_ref[...] = sums / jnp.maximum(jnp.sum(member, axis=1, keepdims=True), 1.0)


def run_layer(layer, lo, kind, x, segc, cos_t, sin_t, gains, weights, more):
    is_first, is_last = layer == 0, layer == N_LAYERS - 1
    vmem = pl.BlockSpec(memory_space=pltpu.VMEM)
    smem = pl.BlockSpec(memory_space=pltpu.SMEM)
    scratch = [
        pltpu.VMEM((32, 4, 16, LAYER_COLS), BF16),
        pltpu.VMEM((2 * N_PAIRS, N_SLOTS, 128), BF16), pltpu.VMEM((2 * N_PAIRS, N_SLOTS + 128, 128), BF16),
        pltpu.VMEM((N_PAIRS, N_SLOTS + 128, 128), BF16), pltpu.VMEM((N_PAIRS, N_SLOTS, 128), BF16), pltpu.VMEM((ROWS, FF_DIM), BF16),
        pltpu.SemaphoreType.DMA((5,)),
    ]
    out_shape = jax.ShapeDtypeStruct((N_SLOTS, D_MODEL), BF16)
    if is_first:
        scratch.append(pltpu.VMEM((32, 4, 16, 512), BF16))
    elif is_last:
        out_shape = jax.ShapeDtypeStruct((DOC_SLOTS, D_MODEL), F32)
        scratch.append(pltpu.VMEM((N_SLOTS, D_MODEL), BF16))
    else:
        scratch.append(pltpu.VMEM((QB, 2 * QB), F32))
    return pl.pallas_call(
        functools.partial(layer_kernel, layer),
        out_shape=out_shape,
        in_specs=[smem, smem] + [vmem] * 5 + [pl.BlockSpec(memory_space=pltpu.HBM)] + [vmem] * len(more),
        out_specs=vmem,
        scratch_shapes=scratch,
        compiler_params=pltpu.CompilerParams(vmem_limit_bytes=VMEM_BYTES),
        cost_estimate=COST,
        name=f"layer_{layer}",
    )(lo, kind, x, segc, cos_t, sin_t, gains, weights, *more)


def meet_kernel(say_ref, qkv_ref, out_ref, in_ref, heard_ref, quart_ref, send_sem, recv_sem, own_sem, w_send, w_recv, w_own):
    me = lax.axis_index("dp")
    mine = lax.rem(me, 4)
    barrier = pltpu.get_barrier_semaphore()

    @pl.loop(1, N_DEV)
    def greet(step):
        pl.semaphore_signal(barrier, inc=1, device_id={"dp": lax.rem(me + step, N_DEV)}, device_id_type=MESH)

    own = [pltpu.make_async_copy(say_ref.at[me], heard_ref.at[me], own_sem)]

    def pieces(quarter, slot):
        out = []
        for part in range(3):
            cols = pl.ds(pl.multiple_of(part * 512 + quarter * 128, 128), 128)
            out.append((qkv_ref.at[:, :, cols], quart_ref.at[slot, :, :, pl.ds(part * 128, 128)]))
        out.append((out_ref.at[:, :, pl.ds(pl.multiple_of(quarter * 128, 128), 128)], quart_ref.at[slot, :, :, pl.ds(384, 128)]))
        for part in range(2):
            cols = pl.ds(pl.multiple_of(part * 2048 + quarter * 512, 512), 512)
            out.append((in_ref.at[:, :, cols], quart_ref.at[slot, :, :, pl.ds(512 + part * 512, 512)]))
        return out

    own += [pltpu.make_async_copy(src, dst, w_own.at[index]) for index, (src, dst) in enumerate(pieces(mine, mine))]
    for copy in own:
        copy.start()
    pl.semaphore_wait(barrier, N_DEV - 1)

    quarters = []
    for step in range(1, 4):
        quarter = lax.rem(mine + step, 4)
        for index, (src, dst) in enumerate(pieces(quarter, mine)):
            number = (step - 1) * 6 + index
            quarters.append(pltpu.make_async_remote_copy(
                src_ref=src, dst_ref=dst, send_sem=w_send.at[number], recv_sem=w_recv.at[number],
                device_id={"dp": me - mine + quarter}, device_id_type=MESH))
    for copy in quarters:
        copy.start()

    @pl.loop(1, N_DEV)
    def tell(step):
        peer = lax.rem(me + step, N_DEV)
        pltpu.make_async_remote_copy(
            src_ref=say_ref.at[peer], dst_ref=heard_ref.at[me], send_sem=send_sem, recv_sem=recv_sem,
            device_id={"dp": peer}, device_id_type=MESH).start()

    rest = pltpu.make_async_remote_copy(
        src_ref=say_ref.at[pl.ds(0, N_DEV - 1)], dst_ref=heard_ref.at[pl.ds(0, N_DEV - 1)], send_sem=send_sem, recv_sem=recv_sem,
        device_id={"dp": lax.rem(me + 1, N_DEV)}, device_id_type=MESH)
    rest.wait_send()
    rest.wait_recv()
    for copy in own + quarters:
        copy.wait()


def meet(say, w_qkv, w_out, w_in):
    vmem = pl.BlockSpec(memory_space=pltpu.VMEM)
    dma = pltpu.SemaphoreType.DMA
    return pl.pallas_call(
        meet_kernel,
        out_shape=(jax.ShapeDtypeStruct(say.shape, F32), jax.ShapeDtypeStruct((4, N_LAYERS, 4, 1536), BF16)),
        in_specs=[vmem] * 4,
        out_specs=(vmem, vmem),
        scratch_shapes=[dma, dma, dma, dma((18,)), dma((18,)), dma((6,))],
        compiler_params=pltpu.CompilerParams(collective_id=1, has_side_effects=True),
        cost_estimate=COST,
        name="meet",
    )(say, w_qkv, w_out, w_in)


COLOR_COLS = ((0, 512, 896), (896, 1408, 1792), (1792, 2176, 2560))
COLOR_DIMS = ((2, 1, 0), (1, 0, 2), (0, 2, 1))
PIECES = ((0, 1),)


def gather_kernel(shard_ref, rows_ref, all_ref, got_ref, send_sem, recv_sem, pair_send, pair_recv, own_sem, row_send, row_recv, row_own):
    me = lax.axis_index("dp")
    core = lax.rem(me, 2)
    place = [lax.div(me, 32), lax.rem(lax.div(me, 8), 4), lax.rem(lax.div(me, 2), 4)]
    stride = (32, 8, 2)

    def neighbour(dim, shift):
        return me + (lax.rem(place[dim] + shift, 4) - place[dim]) * stride[dim]

    partner = me + 1 - 2 * core
    barrier = pltpu.get_barrier_semaphore()

    @pl.loop(1, N_DEV)
    def greet(step):
        pl.semaphore_signal(barrier, inc=1, device_id={"dp": lax.rem(me + step, N_DEV)}, device_id_type=MESH)

    own = pltpu.make_async_copy(shard_ref, all_ref.at[place[0], place[1], place[2], core], own_sem)
    own.start()
    own_rows = pltpu.make_async_copy(rows_ref.at[me], got_ref.at[me], row_own)
    own_rows.start()
    pl.semaphore_wait(barrier, N_DEV - 1)

    def give(part):
        @pl.loop(max(part * 22, 1), min(part * 22 + 22, N_DEV))
        def to_peer(step):
            peer = lax.rem(me + step, N_DEV)
            pltpu.make_async_remote_copy(
                src_ref=rows_ref.at[peer], dst_ref=got_ref.at[me], send_sem=row_send, recv_sem=row_recv,
                device_id={"dp": peer}, device_id_type=MESH).start()

    sent = []

    def block(piece, color, phase, shift, half):
        start, middle, stop = COLOR_COLS[color]
        if half == 0:
            stop = middle
        if half == 1:
            start = middle
        first, count = PIECES[piece]
        if phase < 0:
            return shard_ref.at[pl.ds(first, count), :, pl.ds(start, stop - start)]
        index = list(place)
        for dim in COLOR_DIMS[color][:phase]:
            index[dim] = slice(None)
        dim = COLOR_DIMS[color][phase]
        index[dim] = lax.rem(place[dim] + shift, 4)
        return all_ref.at[index[0], index[1], index[2], core, pl.ds(first, count), :, pl.ds(start, stop - start)]

    def send(src, dst, sems, number, other):
        copy = pltpu.make_async_remote_copy(
            src_ref=src, dst_ref=dst, send_sem=sems[0].at[number], recv_sem=sems[1].at[number],
            device_id={"dp": other}, device_id_type=MESH)
        copy.start()
        sent.append(copy)

    def arrived(region, sems, number):
        pltpu.make_async_remote_copy(
            src_ref=region, dst_ref=region, send_sem=sems[0].at[number], recv_sem=sems[1].at[number],
            device_id={"dp": partner}, device_id_type=MESH).wait_recv()

    ring, pair = (send_sem, recv_sem), (pair_send, pair_recv)
    todo = [(piece, color) for piece in range(len(PIECES)) for color in range(3)]

    def slot(piece, color, phase, kind):
        return ((piece * 3 + color) * 3 + phase) * 4 + kind

    def pair_slot(piece, color, phase, kind):
        return (piece * 3 + color) * 10 + (0 if phase < 0 else 1 + phase * 3 + kind)

    def begin(piece, color, phase):
        dim = COLOR_DIMS[color][phase]
        dst = block(piece, color, phase, 0, None)
        src = block(piece, color, -1, 0, None) if phase == 0 else dst
        send(src, dst, ring, slot(piece, color, phase, 0), neighbour(dim, 1))
        send(src, dst, ring, slot(piece, color, phase, 1), neighbour(dim, 3))
        if phase == 0:
            send(src, dst, pair, pair_slot(piece, color, -1, 0), partner)

    def forward(piece, color, phase):
        dim = COLOR_DIMS[color][phase]
        for kind, shift in ((0, 3), (1, 1)):
            region = block(piece, color, phase, shift, None)
            arrived(region, ring, slot(piece, color, phase, kind))
            part = block(piece, color, phase, shift, kind)
            send(part, part, ring, slot(piece, color, phase, 2 + kind), neighbour(dim, 1 if kind == 0 else 3))
            send(region, region, pair, pair_slot(piece, color, phase, kind), partner)

    def finish(piece, color, phase):
        for kind in (0, 1):
            arrived(block(piece, color, phase, 2, kind), ring, slot(piece, color, phase, 2 + kind))
        region = block(piece, color, phase, 2, None)
        send(region, region, pair, pair_slot(piece, color, phase, 2), partner)

    for piece, color in todo:
        begin(piece, color, 0)
    give(0)
    own.wait()
    for phase in range(3):
        for piece, color in todo:
            forward(piece, color, phase)
        give(1 + 2 * phase)
        for piece, color in todo:
            finish(piece, color, phase)
            if phase < 2:
                begin(piece, color, phase + 1)
        if phase < 2:
            give(2 + 2 * phase)

    for piece, color in todo:
        first, count = PIECES[piece]
        start, _, stop = COLOR_COLS[color]
        tail = (1 - core, pl.ds(first, count), slice(None), pl.ds(start, stop - start))
        arrived(all_ref.at[(place[0], place[1], place[2]) + tail], pair, pair_slot(piece, color, -1, 0))
        for phase in range(3):
            for kind, shift in ((0, 3), (1, 1), (2, 2)):
                index = list(place)
                for dim in COLOR_DIMS[color][:phase]:
                    index[dim] = slice(None)
                dim = COLOR_DIMS[color][phase]
                index[dim] = lax.rem(place[dim] + shift, 4)
                arrived(all_ref.at[tuple(index) + tail], pair, pair_slot(piece, color, phase, kind))
    for copy in sent:
        copy.wait_send()
    rest = pltpu.make_async_remote_copy(
        src_ref=rows_ref.at[pl.ds(0, N_DEV - 1)], dst_ref=got_ref.at[pl.ds(0, N_DEV - 1)], send_sem=row_send, recv_sem=row_recv,
        device_id={"dp": lax.rem(me + 1, N_DEV)}, device_id_type=MESH)
    rest.wait_send()
    rest.wait_recv()
    own_rows.wait()


def gather_near(shard, rows):
    dma = pltpu.SemaphoreType.DMA
    vmem = pl.BlockSpec(memory_space=pltpu.VMEM)
    n_ring, n_pair = len(PIECES) * 36, len(PIECES) * 30
    out, got = pl.pallas_call(
        gather_kernel,
        out_shape=(jax.ShapeDtypeStruct((4, 4, 4, 2) + shard.shape, BF16), jax.ShapeDtypeStruct(rows.shape, BF16)),
        in_specs=[vmem, vmem],
        out_specs=(pl.BlockSpec(memory_space=pltpu.HBM), vmem),
        scratch_shapes=[dma((n_ring,)), dma((n_ring,)), dma((n_pair,)), dma((n_pair,)), dma, dma, dma, dma],
        compiler_params=pltpu.CompilerParams(collective_id=2, has_side_effects=True),
        cost_estimate=COST,
        name="gather",
    )(shard, rows)
    return out.reshape((32, 4) + shard.shape), got.reshape(N_DEV * CAP, D_MODEL)


def exact_dot(a, b):
    return jnp.dot(a, b, precision=lax.Precision.HIGHEST, preferred_element_type=F32)


def plan_requests(tok_ids, seg_ids, shard_rows):
    owner = jnp.where(seg_ids >= 0, tok_ids // shard_rows, -1)
    local = tok_ids % shard_rows
    hot = (owner[:, None] == jnp.arange(N_DEV)[None, :]).astype(BF16)
    earlier = (jnp.arange(N_SLOTS)[:, None] > jnp.arange(N_SLOTS)[None, :]).astype(BF16)
    before = jnp.dot(earlier, hot, preferred_element_type=F32)
    rank = jnp.sum(before * hot.astype(F32), axis=1).astype(jnp.int32)
    counts = jnp.sum(hot.astype(F32), axis=0)
    return owner, local, hot, rank, counts


def ids_to_ask(local, hot, rank, width):
    place = rank[:, None] == jnp.arange(width)[None, :]
    high = jnp.where(place, (local // 32)[:, None], 0).astype(BF16)
    low = jnp.where(place, (local % 32)[:, None], 0).astype(BF16)
    both = lax.dot_general(hot, jnp.concatenate([high, low], axis=1), (((0,), (0,)), ((), ())), preferred_element_type=F32)
    return both[:, :width] * 32.0 + both[:, width:]


def pick_rows(ids, table):
    hot = (ids.reshape(-1, 1) == jnp.arange(table.shape[0]).astype(F32)[None, :]).astype(BF16)
    return jnp.dot(hot, table, preferred_element_type=F32).astype(BF16)


def spilled_rows(asks, wanted, table):
    me = lax.axis_index("dp")
    devs = jnp.arange(N_DEV)
    extra = jnp.maximum(asks - CAP, 0.0)
    sizes = jnp.sum(jnp.where(devs[None, :] == me, extra, 0.0), axis=1)[None, :]
    starts = exact_dot(sizes, (devs[:, None] < devs[None, :]).astype(F32))
    row = jnp.arange(SPILL).astype(F32)[:, None]
    mine = (starts <= row) & (row < starts + sizes)
    rank = jnp.sum(jnp.where(mine, row - starts + CAP, 0.0), axis=1, keepdims=True)
    choice = exact_dot(mine.astype(F32), wanted)
    return pick_rows(jnp.sum(jnp.where(jnp.arange(ASK).astype(F32)[None, :] == rank, choice, 0.0), axis=1), table)


def place_rows(owner, local, hot, rank, asks, table):
    me = lax.axis_index("dp")
    extra = jnp.maximum(asks - CAP, 0.0)
    too_many = (jnp.max(asks) > ASK) | (jnp.max(jnp.sum(extra, axis=0)) > SPILL)
    starts = jnp.sum(jnp.where(jnp.arange(N_DEV)[:, None] < me, extra, 0.0), axis=0)
    base = jnp.sum(hot.astype(F32) * starts[None, :], axis=1).astype(jnp.int32)
    near = jnp.where((owner >= 0) & (rank < CAP), owner * CAP + rank, -1)
    far = jnp.where((owner >= 0) & (rank >= CAP), owner * SPILL + base + rank - CAP, -1)

    def by_rounds():
        def one_round(number, rows):
            here = rank - number * CAP
            ids = lax.all_to_all(ids_to_ask(local, hot, here, CAP), "dp", split_axis=0, concat_axis=0, tiled=True)
            sent = pick_rows(ids, table).reshape(N_DEV, CAP, D_MODEL)
            back = lax.all_to_all(sent, "dp", split_axis=0, concat_axis=0, tiled=True).reshape(N_DEV * CAP, D_MODEL)
            slot = jnp.where((owner >= 0) & (here >= 0) & (here < CAP), owner * CAP + here, -1)
            pick = (slot[:, None] == jnp.arange(N_DEV * CAP)[None, :]).astype(BF16)
            return rows + jnp.dot(pick, back, preferred_element_type=F32).astype(BF16)

        rounds = jnp.ceil(jnp.max(asks) / CAP).astype(jnp.int32)
        return lax.fori_loop(0, rounds, one_round, none())

    def none():
        return jnp.zeros((N_SLOTS, D_MODEL), BF16)

    near = jnp.where(too_many, -1, near)
    far = jnp.where(too_many, -1, far)
    return near[:, None], far[:, None], lax.cond(too_many, by_rounds, none)


def rope_tables(positions, theta):
    inv_freq = theta ** (-jnp.arange(0, HEAD_DIM, 2).astype(F32) / HEAD_DIM)
    angles = positions.astype(F32)[:, None] * jnp.tile(inv_freq, 4)[None, :]
    sign = jnp.where(jnp.arange(128) % HEAD_DIM < HEAD_DIM // 2, -1.0, 1.0)
    return jnp.cos(angles), jnp.sin(angles) * sign[None, :]


def key_ranges(seg_ids, positions):
    n_blocks = N_SLOTS // GLOBAL_QB
    first = jnp.arange(n_blocks) * GLOBAL_QB
    seg_first = seg_ids[::GLOBAL_QB]
    lo = jnp.where(seg_first >= 0, first - positions[::GLOBAL_QB], first) // QB
    last_seg = jnp.max(seg_ids.reshape(n_blocks, GLOBAL_QB), axis=1)
    hi = jnp.sum(((seg_ids >= 0)[None, :] & (seg_ids[None, :] <= last_seg[:, None])).astype(jnp.int32), axis=1)
    span = jnp.maximum(hi - lo * QB, 1)
    kind = jnp.sum((span[:, None] > jnp.array(SPANS)[None, :]).astype(jnp.int32), axis=1)
    return lo.astype(jnp.int32), kind.astype(jnp.int32)


def solution(mesh):
    token_spec = P(("pod", "dp"))
    layer_spec = P(None, "dp", None)
    gain_spec = P(None, "dp")
    in_specs = (token_spec, token_spec, token_spec, P("dp", None), P("dp"), layer_spec, layer_spec, layer_spec, layer_spec, gain_spec, gain_spec, P("dp"))

    def device_program(tok_ids, seg_ids, positions, emb_table, gain_emb, w_qkv, w_out, w_in, w_down, gain_attn, gain_mlp, gain_final):
        owner, local, hot, rank, counts = plan_requests(tok_ids, seg_ids, emb_table.shape[0])
        wanted = ids_to_ask(local, hot, rank, ASK)
        gains = jnp.concatenate([gain_emb[None], gain_attn, gain_mlp, gain_final[None]], axis=0).astype(F32).reshape(1, -1)
        n_gain = gains.shape[1]
        tail = jnp.concatenate([wanted, jnp.broadcast_to(gains, (N_DEV, n_gain)), jnp.zeros((N_DEV, 128 - ASK - n_gain), F32)], axis=1)
        say = jnp.stack([jnp.broadcast_to(counts[None, :], (N_DEV, N_DEV)), tail], axis=1)
        heard, quarters = meet(say, w_qkv, w_out, w_in)
        asks, asked = heard[:, 0, :], heard[:, 1, :ASK]
        shard = jnp.concatenate([quarters.transpose(1, 0, 2, 3).reshape(N_LAYERS, 16, 1536), w_down], axis=2)
        far_weights = lax.all_gather(shard[1:][None], "dp", axis=0, tiled=True).reshape(32, 4, 3, 16, LAYER_COLS)
        spill = spilled_rows(asks, asked, emb_table)[None]
        rows = pick_rows(asked[:, :CAP], emb_table).reshape(N_DEV, CAP, D_MODEL)
        near_weights, hidden = gather_near(jnp.concatenate([shard[:1], spill], axis=2), rows)
        near, far, late = place_rows(owner, local, hot, rank, asks, emb_table)
        gains = heard[:, 1, ASK:ASK + n_gain].reshape(N_DEV, n_gain // 4, 4).transpose(1, 0, 2).reshape(n_gain // 4, D_MODEL)
        segc = seg_ids[:, None]
        lo, kind = key_ranges(seg_ids, positions)
        tables = (rope_tables(positions, THETA_GLOBAL), rope_tables(positions, THETA_LOCAL))
        for layer in range(N_LAYERS):
            cos_t, sin_t = tables[int(layer % 3 != 0)]
            more = [near, far, late] if layer == 0 else [seg_ids[None, :]] if layer == N_LAYERS - 1 else []
            hidden = run_layer(layer, lo, kind, hidden, segc, cos_t, sin_t, gains, near_weights if layer == 0 else far_weights, more)
        return hidden

    return jax.shard_map(device_program, mesh=mesh, in_specs=in_specs, out_specs=P(("pod", "dp"), None), check_vma=False)
```
